32 devices in a mesh: dp: 1 (over z), cp: 4 (over y), tp: 8 (over x, core).
Axes of the slice: x: 4, y: 4, z: 1, core: 2. Of those that a mesh axis runs over, the one named last changes fastest.
The devices are a block of a 4x4x8 slice.
Arguments:
- x: bfloat16 [8192, 2048], P(('dp', 'cp', 'tp'))
- idx: int32 [8192, 2], P(('dp', 'cp', 'tp'))
- gates: float32 [8192, 2], P(('dp', 'cp', 'tp'))
- wq: bfloat16 [2048, 2048], P(None, 'tp')
- wk: bfloat16 [2048, 2048], P(None, 'tp')
- wv: bfloat16 [2048, 2048], P(None, 'tp')
- wo: bfloat16 [2048, 2048], P('tp')
- w1g: bfloat16 [32, 2048, 1408], P(('cp', 'tp'))
- w1u: bfloat16 [32, 2048, 1408], P(('cp', 'tp'))
- w2: bfloat16 [32, 1408, 2048], P(('cp', 'tp'))
Outputs:
- output: bfloat16 [8192, 2048], P(('dp', 'cp', 'tp'))
All inputs are finite; a program needn't handle non-finite values.
Results may differ from the reference program's by a relative error of at most 0.0100242.
Values are sent between devices in bfloat16 or wider.
A program may use at most 768 MiB of HBM per device.

```python
import math
import jax
import jax.numpy as jnp
from jax import lax

H = 2048
FF = 1408
HEADS = 16
KV_HEADS = 16
HEAD = 128
S = 8192
CP = 4
TP = 8
TOP = 2
QBLK = 512

E = CP * TP
T = S // E
CAP = 4 * T // E
M = 2 * T // E


def seg_positions():
    i = jnp.arange(S, dtype=jnp.int32)
    seg = S // (2 * CP)
    b = i // seg
    r = b // 2
    s_id = jnp.where(b % 2 == 0, r, 2 * CP - 1 - r)
    return s_id * seg + i % seg


def source_routing(key, sigma, counts):
    ends = jnp.cumsum(counts)
    labels = sigma[jnp.searchsorted(ends, jnp.arange(2 * T, dtype=jnp.int32), side='right')]
    perm = jax.random.permutation(key, T)
    return jnp.stack([labels[perm], labels[perm + T]], axis=1).astype(jnp.int32)


def setup_inputs(seed: int = 0, part: int = 0) -> dict:
    key = jax.random.key(seed)
    ks = jax.random.split(key, 7)
    kx = jax.random.split(jax.random.fold_in(key, part), 4)
    a = math.log(S / 16.0) ** 0.25

    def nrm(k, shape, scale):
        return (jax.random.normal(k, shape, jnp.float32) * scale).astype(jnp.bfloat16)

    wq = nrm(ks[0], (H, HEADS * HEAD), a / math.sqrt(H))
    wk = nrm(ks[1], (H, KV_HEADS * HEAD), a / math.sqrt(H))
    wv = nrm(ks[2], (H, KV_HEADS * HEAD), 1.0 / math.sqrt(H))
    wo = nrm(ks[3], (HEADS * HEAD, H), 1.0 / math.sqrt(HEADS * HEAD))
    w1g = nrm(ks[4], (E, H, FF), 1.0 / math.sqrt(H))
    w1u = nrm(ks[5], (E, H, FF), 1.0 / math.sqrt(H))
    w2 = nrm(ks[6], (E, FF, H), 1.5 / math.sqrt(FF))
    x = nrm(kx[0], (S, H), 1.0)
    sigmas = jax.vmap(lambda kk: jax.random.permutation(kk, E))(jax.random.split(kx[1], E))
    counts = jnp.full((E,), M, jnp.int32)
    idx = jax.vmap(lambda kk, sg: source_routing(kk, sg, counts))(jax.random.split(kx[2], E), sigmas)
    idx = idx.reshape(S, TOP)
    gates = jax.random.uniform(kx[3], (S, TOP), jnp.float32, 0.3, 0.7)
    return {'x': x, 'idx': idx, 'gates': gates, 'wq': wq, 'wk': wk, 'wv': wv, 'wo': wo, 'w1g': w1g, 'w1u': w1u, 'w2': w2}


def reference(x, idx, gates, wq, wk, wv, wo, w1g, w1u, w2):
    pos = seg_positions()
    g = HEADS // KV_HEADS
    q = jnp.dot(x, wq, preferred_element_type=jnp.float32).astype(jnp.bfloat16)
    k = jnp.dot(x, wk, preferred_element_type=jnp.float32).astype(jnp.bfloat16)
    v = jnp.dot(x, wv, preferred_element_type=jnp.float32).astype(jnp.bfloat16)
    qh = q.reshape(S, HEADS, HEAD).transpose(1, 0, 2)
    kh = jnp.repeat(k.reshape(S, KV_HEADS, HEAD).transpose(1, 0, 2), g, axis=0)
    vh = jnp.repeat(v.reshape(S, KV_HEADS, HEAD).transpose(1, 0, 2), g, axis=0)
    scale = HEAD ** -0.5
    nb = S // QBLK

    def head(args):
        qa, ka, va = args

        def block(bargs):
            qb, pb = bargs
            s = jnp.dot(qb, ka.T, preferred_element_type=jnp.float32) * scale
            mask = pos[None, :] <= pb[:, None]
            s = jnp.where(mask, s, -1e30)
            m = jnp.max(s, axis=-1, keepdims=True)
            w = jnp.where(mask, jnp.exp(s - m), 0.0)
            l = jnp.sum(w, axis=-1, keepdims=True)
            ob = jnp.dot(w.astype(jnp.bfloat16), va, preferred_element_type=jnp.float32)
            return ob / l

        out = lax.map(block, (qa.reshape(nb, QBLK, HEAD), pos.reshape(nb, QBLK)))
        return out.reshape(S, HEAD)

    o = lax.map(head, (qh, kh, vh))
    o = o.transpose(1, 0, 2).reshape(S, HEADS * HEAD).astype(jnp.bfloat16)
    att = jnp.dot(o, wo, preferred_element_type=jnp.float32)
    h = (x.astype(jnp.float32) + att).astype(jnp.bfloat16)

    ea = idx.reshape(-1)
    tok = jnp.arange(S * TOP) // TOP
    onehot = (ea[:, None] == jnp.arange(E)[None, :]).astype(jnp.int32)
    slot = jnp.take_along_axis(jnp.cumsum(onehot, axis=0), ea[:, None], axis=1)[:, 0] - 1
    ct = E * CAP
    buf = jnp.zeros((E, ct, H), jnp.bfloat16).at[ea, slot].set(h[tok])

    def expert(args):
        rows, wg, wu, wd = args
        gg = jnp.dot(rows, wg, preferred_element_type=jnp.float32)
        uu = jnp.dot(rows, wu, preferred_element_type=jnp.float32)
        act = (jax.nn.silu(gg) * uu).astype(jnp.bfloat16)
        return jnp.dot(act, wd, preferred_element_type=jnp.float32).astype(jnp.bfloat16)

    z = lax.map(expert, (buf, w1g, w1u, w2))
    zt = z[ea, slot].astype(jnp.float32).reshape(S, TOP, H)
    y = h.astype(jnp.float32) + jnp.sum(gates[:, :, None] * zt, axis=1)
    return y.astype(jnp.bfloat16)
```

```python
import functools

import jax
import jax.numpy as jnp
from jax import lax
from jax.experimental import pallas as pl
from jax.experimental.pallas import tpu as pltpu
from jax.sharding import PartitionSpec as P

HEAD_DIM = 128
NEG = -1e30
LOG2E = 1.4426950408889634
MESH = pl.DeviceIdType.MESH
HALF = 128
LAG = 3


def greet(cp, tp, c, t):
    sem = pltpu.get_barrier_semaphore()
    n = 0
    for dc in range(cp):
        for dt in range(tp):
            if dc or dt:
                peer = {'cp': lax.rem(c + dc, cp), 'tp': lax.rem(t + dt, tp)}
                pl.semaphore_signal(sem, inc=1, device_id=peer, device_id_type=MESH)
                n += 1
    pl.semaphore_wait(sem, n)


def project_kernel(cp, tp, x_ref, wq_ref, wk_ref, wv_ref, out_ref, xs, stage,
                   ss_x, ss_f, rs_x, sy, ry, sf, rf, sl):
    c = lax.axis_index('cp')
    t = lax.axis_index('tp')
    nx = tp // 2
    X = t // 2
    i = lax.rem(t, 2)
    partner = {'cp': c, 'tp': 2 * X + 1 - i}
    main = i == c // 2
    greet(cp, tp, c, t)

    def rows(hf):
        return pl.ds(pl.multiple_of(hf * HALF, HALF), HALF)

    def own_send(d, hf):
        if d == 0:
            dev, u, w = partner, 0, 1
        else:
            dev = {'cp': c, 'tp': 2 * lax.rem(X + d, nx) + i}
            u, w = {1: 2, 3: 1, 2: 3}[d], 0
        return pltpu.make_async_remote_copy(
            src_ref=x_ref.at[rows(hf)], dst_ref=xs.at[t, rows(hf)],
            send_sem=ss_x.at[d * 2 + hf], recv_sem=rs_x.at[u * 4 + w * 2 + hf],
            device_id=dev, device_id_type=MESH)

    def source(u, w):
        dx = u + (u // 2) * (5 - 2 * u)
        return 2 * lax.rem(X + dx, nx) + lax.rem(i + w, 2)

    def forward(u, hf):
        s = source(u, 0)
        return pltpu.make_async_remote_copy(
            src_ref=xs.at[s, rows(hf)], dst_ref=xs.at[s, rows(hf)],
            send_sem=ss_f.at[u * 2 + hf], recv_sem=rs_x.at[u * 4 + 2 + hf],
            device_id=partner, device_id_type=MESH)

    def landed(u, w, hf):
        s = source(u, w)
        return pltpu.make_async_remote_copy(
            src_ref=xs.at[s, rows(hf)], dst_ref=xs.at[s, rows(hf)],
            send_sem=ss_f.at[u * 2 + hf], recv_sem=rs_x.at[u * 4 + w * 2 + hf],
            device_id=partner, device_id_type=MESH)

    def place(cc, s, hf):
        seg = cc + (s // 4) * (2 * cp - 1 - 2 * cc)
        return pl.ds(pl.multiple_of(seg * 1024 + lax.rem(s, 4) * 256 + hf * HALF, HALF), HALF)

    def step_of(q):
        first = (q // 2 == 0)
        r = q - 2
        ge = r // 4
        hf = (1 - ge) * (r // 2) + ge * (r - 4)
        u = (1 - ge) * (1 + lax.rem(r, 2)) + ge * 3
        del first
        return u, hf

    def y_send(p, kk, s, hf):
        return pltpu.make_async_remote_copy(
            src_ref=stage.at[p, kk], dst_ref=out_ref.at[place(c, s, hf)],
            send_sem=sy.at[p * 2 + kk], recv_sem=ry.at[c * 16 + p],
            device_id={'cp': 2 * i + kk, 'tp': t}, device_id_type=MESH)

    def keep(p, kk, s, hf):
        return pltpu.make_async_copy(stage.at[p, kk], out_ref.at[place(c, s, hf)], sl.at[p])

    def share(p, kk, s, hf):
        return pltpu.make_async_remote_copy(
            src_ref=stage.at[p, kk], dst_ref=out_ref.at[place(c, s, hf)],
            send_sem=sf.at[c * 16 + p], recv_sem=rf.at[c * 16 + p],
            device_id=partner, device_id_type=MESH)

    def pass_on(cc, p, s, hf):
        return pltpu.make_async_remote_copy(
            src_ref=out_ref.at[place(cc, s, hf)], dst_ref=out_ref.at[place(cc, s, hf)],
            send_sem=sf.at[cc * 16 + p], recv_sem=rf.at[cc * 16 + p],
            device_id=partner, device_id_type=MESH)

    def y_landed(cc, p, s, hf):
        return pltpu.make_async_remote_copy(
            src_ref=out_ref.at[place(cc, s, hf)], dst_ref=out_ref.at[place(cc, s, hf)],
            send_sem=sf.at[cc * 16 + p], recv_sem=ry.at[cc * 16 + p],
            device_id=partner, device_id_type=MESH)

    for hf in range(2):
        for d in (1, 3, 0):
            own_send(d, hf).start()
    for hf in range(2):
        own_send(2, hf).start()

    def project(xv, p, s, hf):
        for n, w_ref in enumerate((wq_ref, wk_ref, wv_ref)):
            r = jnp.dot(xv, w_ref[...], preferred_element_type=jnp.float32).astype(jnp.bfloat16)
            for kk in range(2):
                stage[p, kk, :, n * HEAD_DIM:(n + 1) * HEAD_DIM] = r[:, kk * HEAD_DIM:(kk + 1) * HEAD_DIM]
        for kk in range(2):
            here = c == 2 * i + kk

            @pl.when(jnp.logical_not(here))
            def _():
                y_send(p, kk, s, hf).start()

            @pl.when(here)
            def _():
                keep(p, kk, s, hf).start()
                share(p, kk, s, hf).start()

    def relay(p, s, hf):
        @pl.when(main)
        def _():
            for d in range(1, cp):
                cc = lax.rem(c + d, cp)
                y_landed(cc, p, s, hf).wait_recv()
                pass_on(cc, p, s, hf).start()

    def step0(q, _):
        project(x_ref[rows(q), :], 2 * q, t, q)
        landed(0, 1, q).wait_recv()
        s = source(0, 1)
        project(xs[s, rows(q), :], 2 * q + 1, s, q)
        return 0

    lax.fori_loop(0, 2, step0, 0)

    def late(q):
        u, hf = step_of(q)
        relay(2 * q, source(u, 0), hf)
        relay(2 * q + 1, source(u, 1), hf)

    def step(q, _):
        u, hf = step_of(q)
        landed(u, 0, hf).wait_recv()
        forward(u, hf).start()
        s = source(u, 0)
        project(xs[s, rows(hf), :], 2 * q, s, hf)
        landed(u, 1, hf).wait_recv()
        s = source(u, 1)
        project(xs[s, rows(hf), :], 2 * q + 1, s, hf)

        @pl.when(q < 4)
        def _():
            relay(2 * (q - 2), t, q - 2)
            relay(2 * (q - 2) + 1, source(0, 1), q - 2)

        @pl.when(q >= 4)
        def _():
            late(q - 2)
        return 0

    lax.fori_loop(2, 8, step, 0)

    def tail(q, _):
        late(q)
        return 0

    lax.fori_loop(6, 8, tail, 0)

    for hf in range(2):
        for d in range(4):
            own_send(d, hf).wait_send()

    def drain(q, _):
        u, hf = step_of(q)
        forward(u, hf).wait_send()
        return 0

    lax.fori_loop(2, 8, drain, 0)

    def drain_pieces(p, _):
        q = p // 2
        for kk in range(2):
            here = c == 2 * i + kk

            @pl.when(jnp.logical_not(here))
            def _():
                y_send(p, kk, t, 0).wait_send()

            @pl.when(here)
            def _():
                keep(p, kk, t, 0).wait()
        del q

        @pl.when(main)
        def _():
            for cc in range(cp):
                pass_on(cc, p, t, 0).wait_send()

        @pl.when(jnp.logical_not(main))
        def _():
            for cc in range(cp):
                @pl.when(p < 4)
                def _():
                    pass_on(cc, p, lax.rem(p, 2) * (source(0, 1) - t) + t, p // 2).wait_recv()

                @pl.when(p >= 4)
                def _():
                    u, hf = step_of(p // 2)
                    pass_on(cc, p, source(u, lax.rem(p, 2)), hf).wait_recv()
        return 0

    lax.fori_loop(0, 16, drain_pieces, 0)


def project_exchange(x, wq, wk, wv, cp, tp):
    seq = x.shape[0] * cp * tp
    hd = x.shape[1]
    vm = pl.BlockSpec(memory_space=pltpu.VMEM)
    dma = pltpu.SemaphoreType.DMA
    return pl.pallas_call(
        functools.partial(project_kernel, cp, tp),
        out_shape=jax.ShapeDtypeStruct((seq, 3 * HEAD_DIM), jnp.bfloat16),
        in_specs=[vm] * 4,
        out_specs=pl.BlockSpec(memory_space=pl.ANY),
        scratch_shapes=[
            pltpu.VMEM((tp,) + x.shape, jnp.bfloat16),
            pltpu.VMEM((16, 2, HALF, 3 * HEAD_DIM), jnp.bfloat16),
            dma((8,)), dma((8,)), dma((16,)), dma((32,)), dma((64,)), dma((64,)), dma((64,)), dma((16,)),
        ],
        compiler_params=pltpu.CompilerParams(collective_id=0, has_side_effects=True, vmem_limit_bytes=48 << 20),
        name='project_exchange',
    )(x, wq, wk, wv)


QB = 256
KB = 512


def q_block(g, i):
    return 4 * (g // 2) + (1 - i) * 3 * lax.rem(g, 2) + i * (1 + lax.rem(g, 2))


def attention_kernel(qkv_ref, o_ref):
    g = pl.program_id(0)
    i = lax.rem(lax.axis_index('tp'), 2)
    b = q_block(g, i)
    q = qkv_ref[pl.ds(pl.multiple_of(b * QB, QB), QB), 0:HEAD_DIM]
    scale = HEAD_DIM ** -0.5 * LOG2E

    def chunk(off, m, l, acc, masked):
        k = qkv_ref[pl.ds(off, KB), HEAD_DIM:2 * HEAD_DIM]
        v = qkv_ref[pl.ds(off, KB), 2 * HEAD_DIM:3 * HEAD_DIM]
        s = lax.dot_general(q, k, (((1,), (1,)), ((), ())), preferred_element_type=jnp.float32) * scale
        if masked:
            qp = b * QB + lax.broadcasted_iota(jnp.int32, (QB, KB), 0)
            kp = off + lax.broadcasted_iota(jnp.int32, (QB, KB), 1)
            s = jnp.where(kp <= qp, s, NEG)
        mn = jnp.max(s, axis=1, keepdims=True)
        if m is not None:
            mn = jnp.maximum(m, mn)
        w = jnp.exp2(s - mn)
        ls = w[:, 0:128]
        for n in range(1, KB // 128):
            ls = ls + w[:, n * 128:(n + 1) * 128]
        pv = jnp.dot(w.astype(jnp.bfloat16), v, preferred_element_type=jnp.float32)
        if m is None:
            return mn, ls, pv
        c = jnp.exp2(m - mn)
        return mn, l * c + ls, acc * c + pv

    full = b // 2
    m, l, acc = chunk(pl.multiple_of(full * KB, KB), None, None, None, True)

    def body(j, carry):
        return chunk(pl.multiple_of(j * KB, KB), *carry, False)

    m, l, acc = lax.fori_loop(0, full, body, (m, l, acc))
    o_ref[0] = (acc / jnp.sum(l, axis=1, keepdims=True)).astype(jnp.bfloat16)


def attention(qkv):
    seq = qkv.shape[0]
    nb = seq // QB // 2
    return pl.pallas_call(
        attention_kernel,
        out_shape=jax.ShapeDtypeStruct((nb, QB, HEAD_DIM), jnp.bfloat16),
        grid=(nb,),
        in_specs=[pl.BlockSpec((seq, 3 * HEAD_DIM), lambda g: (0, 0))],
        out_specs=pl.BlockSpec((1, QB, HEAD_DIM), lambda g: (g, 0, 0)),
        compiler_params=pltpu.CompilerParams(vmem_limit_bytes=48 << 20),
        cost_estimate=pl.CostEstimate(flops=40_000_000_000, bytes_accessed=8 << 20, transcendentals=1 << 24),
        name='attention',
    )(qkv)


def spread_kernel(cp, tp, o_ref, out_ref, ss, rs, sl):
    c = lax.axis_index('cp')
    t = lax.axis_index('tp')
    X = t // 2
    i = lax.rem(t, 2)
    head = X * cp + c
    greet(cp, tp, c, t)
    nb = o_ref.shape[0]

    def owner(g):
        b = q_block(g, i)
        seg = b // 4
        up = seg // cp
        return seg + up * (2 * cp - 1 - 2 * seg), lax.rem(b, 4) + 4 * up

    def cols(h):
        return pl.ds(pl.multiple_of(h * HEAD_DIM, HEAD_DIM), HEAD_DIM)

    def send(g):
        oc, ot = owner(g)
        return pltpu.make_async_remote_copy(
            src_ref=o_ref.at[g], dst_ref=out_ref.at[:, cols(head)], send_sem=ss.at[g], recv_sem=rs.at[head],
            device_id={'cp': oc, 'tp': ot}, device_id_type=MESH)

    def local(g):
        return pltpu.make_async_copy(o_ref.at[g], out_ref.at[:, cols(head)], sl)

    def mine(g):
        oc, ot = owner(g)
        return jnp.logical_and(oc == c, ot == t)

    for n in range(nb):
        g = lax.rem(n * 5 + head, nb)

        @pl.when(mine(g))
        def _():
            local(g).start()

        @pl.when(jnp.logical_not(mine(g)))
        def _():
            send(g).start()

    for g in range(nb):
        @pl.when(mine(g))
        def _():
            local(g).wait()

        @pl.when(jnp.logical_not(mine(g)))
        def _():
            send(g).wait_send()
    r = lax.rem(t, 4)
    core = lax.rem((r + 1) // 2, 2)
    for h in range(nb):
        here = jnp.logical_and(h == head, core == i)

        @pl.when(jnp.logical_not(here))
        def _():
            pltpu.make_async_remote_copy(
                src_ref=o_ref.at[0], dst_ref=out_ref.at[:, cols(h)], send_sem=ss.at[0], recv_sem=rs.at[h],
                device_id={'cp': c, 'tp': 2 * X + 1 - i}, device_id_type=MESH).wait_recv()


def spread(o, cp, tp):
    nb, rows, hd = o.shape
    vm = pl.BlockSpec(memory_space=pltpu.VMEM)
    dma = pltpu.SemaphoreType.DMA
    return pl.pallas_call(
        functools.partial(spread_kernel, cp, tp),
        out_shape=jax.ShapeDtypeStruct((rows, nb * hd), jnp.bfloat16),
        in_specs=[vm],
        out_specs=vm,
        scratch_shapes=[dma((nb,)), dma((nb,)), dma],
        compiler_params=pltpu.CompilerParams(collective_id=1, has_side_effects=True),
        name='spread',
    )(o)


def expert_ffn(rows, wg, wu, wd):
    gg = jnp.dot(rows, wg, preferred_element_type=jnp.float32)
    uu = jnp.dot(rows, wu, preferred_element_type=jnp.float32)
    act = (jax.nn.silu(gg) * uu).astype(jnp.bfloat16)
    return jnp.dot(act, wd, preferred_element_type=jnp.float32).astype(jnp.bfloat16)


def routes(idx, ne, cap):
    t = idx.shape[0]
    e = jnp.arange(ne)[None, :]
    o0 = (idx[:, 0:1] == e).astype(jnp.bfloat16)
    o1 = (idx[:, 1:2] == e).astype(jnp.bfloat16)
    tri = (jnp.arange(t)[:, None] >= jnp.arange(t)[None, :]).astype(jnp.bfloat16)
    both = jnp.dot(tri, jnp.concatenate([o0, o1], axis=1), preferred_element_type=jnp.float32)
    c0 = both[:, :ne]
    c1 = both[:, ne:] + both[t - 1:, :ne]
    s0 = jnp.sum(o0.astype(jnp.float32) * c0, axis=1).astype(jnp.int32) - 1
    s1 = jnp.sum(o1.astype(jnp.float32) * c1, axis=1).astype(jnp.int32) - 1
    return idx[:, 0] * cap + s0, idx[:, 1] * cap + s1


def solution(mesh):
    cp = mesh.shape['cp']
    tp = mesh.shape['tp']
    ne = cp * tp
    rows_spec = P(('dp', 'cp', 'tp'), None)
    exp_spec = P(('cp', 'tp'), None, None)

    def local(x, idx, gates, wq, wk, wv, wo, w1g, w1u, w2):
        t, hd = x.shape
        cap = 4 * t // ne
        d0, d1 = routes(idx, ne, cap)
        qkv = project_exchange(x, wq, wk, wv, cp, tp)
        qkv, wo = lax.optimization_barrier((qkv, wo))
        wo_all = lax.all_gather(wo, 'tp', axis=0, tiled=True)
        o = spread(attention(qkv), cp, tp)
        att = jnp.dot(o, wo_all, preferred_element_type=jnp.float32)
        h = (x.astype(jnp.float32) + att).astype(jnp.bfloat16)
        places = jnp.arange(ne * cap)
        pick = jnp.logical_or(places[:, None] == d0[None, :], places[:, None] == d1[None, :]).astype(jnp.bfloat16)
        send = jnp.dot(pick, h, preferred_element_type=jnp.float32).astype(jnp.bfloat16).reshape(ne, cap, hd)
        recv = lax.all_to_all(send, ('cp', 'tp'), 0, 0, tiled=True)
        z = expert_ffn(recv.reshape(ne * cap, hd), w1g[0], w1u[0], w2[0])
        back = lax.all_to_all(z.reshape(ne, cap, hd), ('cp', 'tp'), 0, 0, tiled=True).reshape(ne * cap, hd)
        z0 = jnp.dot((d0[:, None] == places[None, :]).astype(jnp.bfloat16), back, preferred_element_type=jnp.float32)
        z1 = jnp.dot((d1[:, None] == places[None, :]).astype(jnp.bfloat16), back, preferred_element_type=jnp.float32)
        y = h.astype(jnp.float32) + gates[:, 0:1] * z0 + gates[:, 1:2] * z1
        return y.astype(jnp.bfloat16)

    return jax.shard_map(local, mesh=mesh, in_specs=(rows_spec, rows_spec, rows_spec, P(None, 'tp'), P(None, 'tp'), P(None, 'tp'), P('tp', None), exp_spec, exp_spec, exp_spec), out_specs=rows_spec, check_vma=False)
```

```python
import functools

import jax
import jax.numpy as jnp
from jax import lax
from jax.experimental import pallas as pl
from jax.experimental.pallas import tpu as pltpu
from jax.sharding import PartitionSpec as P

HEAD_DIM = 128
NEG = -1e30
LOG2E = 1.4426950408889634
MESH = pl.DeviceIdType.MESH
HALF = 128
LAG = 3


def greet(cp, tp, c, t):
    sem = pltpu.get_barrier_semaphore()
    n = 0
    for dc in range(cp):
        for dt in range(tp):
            if dc or dt:
                peer = {'cp': lax.rem(c + dc, cp), 'tp': lax.rem(t + dt, tp)}
                pl.semaphore_signal(sem, inc=1, device_id=peer, device_id_type=MESH)
                n += 1
    pl.semaphore_wait(sem, n)


def project_kernel(cp, tp, x_ref, wq_ref, wk_ref, wv_ref, out_ref, xs, stage,
                   ss_x, ss_f, rs_x, sy, ry, sf, rf, sl):
    c = lax.axis_index('cp')
    t = lax.axis_index('tp')
    nx = tp // 2
    X = t // 2
    i = lax.rem(t, 2)
    partner = {'cp': c, 'tp': 2 * X + 1 - i}
    main = i == c // 2
    greet(cp, tp, c, t)

    def rows(hf):
        return pl.ds(pl.multiple_of(hf * HALF, HALF), HALF)

    def own_send(d, hf):
        if d == 0:
            dev, u, w = partner, 0, 1
        else:
            dev = {'cp': c, 'tp': 2 * lax.rem(X + d, nx) + i}
            u, w = {1: 2, 3: 1, 2: 3}[d], 0
        return pltpu.make_async_remote_copy(
            src_ref=x_ref.at[rows(hf)], dst_ref=xs.at[t, rows(hf)],
            send_sem=ss_x.at[d * 2 + hf], recv_sem=rs_x.at[u * 4 + w * 2 + hf],
            device_id=dev, device_id_type=MESH)

    def source(u, w):
        dx = u + (u // 2) * (5 - 2 * u)
        return 2 * lax.rem(X + dx, nx) + lax.rem(i + w, 2)

    def forward(u, hf):
        s = source(u, 0)
        return pltpu.make_async_remote_copy(
            src_ref=xs.at[s, rows(hf)], dst_ref=xs.at[s, rows(hf)],
            send_sem=ss_f.at[u * 2 + hf], recv_sem=rs_x.at[u * 4 + 2 + hf],
            device_id=partner, device_id_type=MESH)

    def landed(u, w, hf):
        s = source(u, w)
        return pltpu.make_async_remote_copy(
            src_ref=xs.at[s, rows(hf)], dst_ref=xs.at[s, rows(hf)],
            send_sem=ss_f.at[u * 2 + hf], recv_sem=rs_x.at[u * 4 + w * 2 + hf],
            device_id=partner, device_id_type=MESH)

    def place(cc, s, hf):
        seg = cc + (s // 4) * (2 * cp - 1 - 2 * cc)
        return pl.ds(pl.multiple_of(seg * 1024 + lax.rem(s, 4) * 256 + hf * HALF, HALF), HALF)

    def step_of(q):
        first = (q // 2 == 0)
        r = q - 2
        ge = r // 4
        hf = (1 - ge) * (r // 2) + ge * (r - 4)
        u = (1 - ge) * (1 + lax.rem(r, 2)) + ge * 3
        del first
        return u, hf

    def y_send(p, kk, s, hf):
        return pltpu.make_async_remote_copy(
            src_ref=stage.at[p, kk], dst_ref=out_ref.at[place(c, s, hf)],
            send_sem=sy.at[p * 2 + kk], recv_sem=ry.at[c * 16 + p],
            device_id={'cp': 2 * i + kk, 'tp': t}, device_id_type=MESH)

    def keep(p, kk, s, hf):
        return pltpu.make_async_copy(stage.at[p, kk], out_ref.at[place(c, s, hf)], sl.at[p])

    def share(p, kk, s, hf):
        return pltpu.make_async_remote_copy(
            src_ref=stage.at[p, kk], dst_ref=out_ref.at[place(c, s, hf)],
            send_sem=sf.at[c * 16 + p], recv_sem=rf.at[c * 16 + p],
            device_id=partner, device_id_type=MESH)

    def pass_on(cc, p, s, hf):
        return pltpu.make_async_remote_copy(
            src_ref=out_ref.at[place(cc, s, hf)], dst_ref=out_ref.at[place(cc, s, hf)],
            send_sem=sf.at[cc * 16 + p], recv_sem=rf.at[cc * 16 + p],
            device_id=partner, device_id_type=MESH)

    def y_landed(cc, p, s, hf):
        return pltpu.make_async_remote_copy(
            src_ref=out_ref.at[place(cc, s, hf)], dst_ref=out_ref.at[place(cc, s, hf)],
            send_sem=sf.at[cc * 16 + p], recv_sem=ry.at[cc * 16 + p],
            device_id=partner, device_id_type=MESH)

    for hf in range(2):
        for d in (1, 3, 0):
            own_send(d, hf).start()
    for hf in range(2):
        own_send(2, hf).start()

    def project(xv, p, s, hf):
        for n, w_ref in enumerate((wq_ref, wk_ref, wv_ref)):
            r = jnp.dot(xv, w_ref[...], preferred_element_type=jnp.float32).astype(jnp.bfloat16)
            for kk in range(2):
                stage[p, kk, :, n * HEAD_DIM:(n + 1) * HEAD_DIM] = r[:, kk * HEAD_DIM:(kk + 1) * HEAD_DIM]
        for kk in range(2):
            here = c == 2 * i + kk

            @pl.when(jnp.logical_not(here))
            def _():
                y_send(p, kk, s, hf).start()

            @pl.when(here)
            def _():
                keep(p, kk, s, hf).start()
                share(p, kk, s, hf).start()

    def relay(p, s, hf):
        @pl.when(main)
        def _():
            for d in range(1, cp):
                cc = lax.rem(c + d, cp)
                y_landed(cc, p, s, hf).wait_recv()
                pass_on(cc, p, s, hf).start()

    def step0(q, _):
        project(x_ref[rows(q), :], 2 * q, t, q)
        landed(0, 1, q).wait_recv()
        s = source(0, 1)
        project(xs[s, rows(q), :], 2 * q + 1, s, q)
        return 0

    lax.fori_loop(0, 2, step0, 0)

    def late(q):
        u, hf = step_of(q)
        relay(2 * q, source(u, 0), hf)
        relay(2 * q + 1, source(u, 1), hf)

    def step(q, _):
        u, hf = step_of(q)
        landed(u, 0, hf).wait_recv()
        forward(u, hf).start()
        s = source(u, 0)
        project(xs[s, rows(hf), :], 2 * q, s, hf)
        landed(u, 1, hf).wait_recv()
        s = source(u, 1)
        project(xs[s, rows(hf), :], 2 * q + 1, s, hf)

        @pl.when(q < 4)
        def _():
            relay(2 * (q - 2), t, q - 2)
            relay(2 * (q - 2) + 1, source(0, 1), q - 2)

        @pl.when(q >= 4)
        def _():
            late(q - 2)
        return 0

    lax.fori_loop(2, 8, step, 0)

    def tail(q, _):
        late(q)
        return 0

    lax.fori_loop(6, 8, tail, 0)

    for hf in range(2):
        for d in range(4):
            own_send(d, hf).wait_send()

    def drain(q, _):
        u, hf = step_of(q)
        forward(u, hf).wait_send()
        return 0

    lax.fori_loop(2, 8, drain, 0)

    def drain_pieces(p, _):
        q = p // 2
        for kk in range(2):
            here = c == 2 * i + kk

            @pl.when(jnp.logical_not(here))
            def _():
                y_send(p, kk, t, 0).wait_send()

            @pl.when(here)
            def _():
                keep(p, kk, t, 0).wait()
        del q

        @pl.when(main)
        def _():
            for cc in range(cp):
                pass_on(cc, p, t, 0).wait_send()

        @pl.when(jnp.logical_not(main))
        def _():
            for cc in range(cp):
                @pl.when(p < 4)
                def _():
                    pass_on(cc, p, lax.rem(p, 2) * (source(0, 1) - t) + t, p // 2).wait_recv()

                @pl.when(p >= 4)
                def _():
                    u, hf = step_of(p // 2)
                    pass_on(cc, p, source(u, lax.rem(p, 2)), hf).wait_recv()
        return 0

    lax.fori_loop(0, 16, drain_pieces, 0)


def project_exchange(x, wq, wk, wv, cp, tp):
    seq = x.shape[0] * cp * tp
    hd = x.shape[1]
    vm = pl.BlockSpec(memory_space=pltpu.VMEM)
    dma = pltpu.SemaphoreType.DMA
    return pl.pallas_call(
        functools.partial(project_kernel, cp, tp),
        out_shape=jax.ShapeDtypeStruct((seq, 3 * HEAD_DIM), jnp.bfloat16),
        in_specs=[vm] * 4,
        out_specs=pl.BlockSpec(memory_space=pl.ANY),
        scratch_shapes=[
            pltpu.VMEM((tp,) + x.shape, jnp.bfloat16),
            pltpu.VMEM((16, 2, HALF, 3 * HEAD_DIM), jnp.bfloat16),
            dma((8,)), dma((8,)), dma((16,)), dma((32,)), dma((64,)), dma((64,)), dma((64,)), dma((16,)),
        ],
        compiler_params=pltpu.CompilerParams(collective_id=0, has_side_effects=True, vmem_limit_bytes=48 << 20),
        name='project_exchange',
    )(x, wq, wk, wv)


QB = 256
KB = 1024


def q_block(g, i):
    return 4 * (g // 2) + (1 - i) * 3 * lax.rem(g, 2) + i * (1 + lax.rem(g, 2))


def attention_kernel(qkv_ref, o_ref):
    seg = pl.program_id(0)
    i = lax.rem(lax.axis_index('tp'), 2)
    blocks = [q_block(2 * seg + n, i) for n in range(2)]
    q = jnp.concatenate([qkv_ref[pl.ds(pl.multiple_of(b * QB, QB), QB), 0:HEAD_DIM] for b in blocks], axis=0)
    scale = HEAD_DIM ** -0.5 * LOG2E

    def chunk(j, m, l, acc, masked):
        off = pl.multiple_of(j * KB, KB)
        k = qkv_ref[pl.ds(off, KB), HEAD_DIM:2 * HEAD_DIM]
        v = qkv_ref[pl.ds(off, KB), 2 * HEAD_DIM:3 * HEAD_DIM]
        s = lax.dot_general(q, k, (((1,), (1,)), ((), ())), preferred_element_type=jnp.float32) * scale
        if masked:
            row = lax.broadcasted_iota(jnp.int32, (2 * QB, KB), 0)
            qp = jnp.where(row < QB, blocks[0] * QB + row, (blocks[1] - 1) * QB + row)
            kp = off + lax.broadcasted_iota(jnp.int32, (2 * QB, KB), 1)
            s = jnp.where(kp <= qp, s, NEG)
        mn = s[:, 0:128]
        for n in range(1, KB // 128):
            mn = jnp.maximum(mn, s[:, n * 128:(n + 1) * 128])
        mn = jnp.max(mn, axis=1, keepdims=True)
        if m is not None:
            mn = jnp.maximum(m, mn)
        w = jnp.exp2(s - mn)
        ls = w[:, 0:128]
        for n in range(1, KB // 128):
            ls = ls + w[:, n * 128:(n + 1) * 128]
        pv = jnp.dot(w.astype(jnp.bfloat16), v, preferred_element_type=jnp.float32)
        if m is None:
            return mn, ls, pv
        c = jnp.exp2(m - mn)
        return mn, l * c + ls, acc * c + pv

    first = chunk(seg, None, None, None, True)
    m, l, acc = lax.fori_loop(0, seg, lambda j, carry: chunk(j, *carry, False), first)
    o = (acc / jnp.sum(l, axis=1, keepdims=True)).astype(jnp.bfloat16)
    o_ref[0] = o[:QB]
    o_ref[1] = o[QB:]


def attention(qkv):
    seq = qkv.shape[0]
    nb = seq // QB // 2
    return pl.pallas_call(
        attention_kernel,
        out_shape=jax.ShapeDtypeStruct((nb, QB, HEAD_DIM), jnp.bfloat16),
        grid=(nb // 2,),
        in_specs=[pl.BlockSpec((seq, 3 * HEAD_DIM), lambda g: (0, 0))],
        out_specs=pl.BlockSpec((2, QB, HEAD_DIM), lambda g: (g, 0, 0)),
        compiler_params=pltpu.CompilerParams(vmem_limit_bytes=48 << 20),
        cost_estimate=pl.CostEstimate(flops=40_000_000_000, bytes_accessed=8 << 20, transcendentals=1 << 24),
        name='attention',
    )(qkv)


def spread_kernel(cp, tp, o_ref, out_ref, ss, rs, sl):
    c = lax.axis_index('cp')
    t = lax.axis_index('tp')
    X = t // 2
    i = lax.rem(t, 2)
    head = X * cp + c
    greet(cp, tp, c, t)
    nb = o_ref.shape[0]

    def owner(g):
        b = q_block(g, i)
        seg = b // 4
        up = seg // cp
        return seg + up * (2 * cp - 1 - 2 * seg), lax.rem(b, 4) + 4 * up

    def cols(h):
        return pl.ds(pl.multiple_of(h * HEAD_DIM, HEAD_DIM), HEAD_DIM)

    def send(g):
        oc, ot = owner(g)
        return pltpu.make_async_remote_copy(
            src_ref=o_ref.at[g], dst_ref=out_ref.at[:, cols(head)], send_sem=ss.at[g], recv_sem=rs.at[head],
            device_id={'cp': oc, 'tp': ot}, device_id_type=MESH)

    def local(g):
        return pltpu.make_async_copy(o_ref.at[g], out_ref.at[:, cols(head)], sl)

    def mine(g):
        oc, ot = owner(g)
        return jnp.logical_and(oc == c, ot == t)

    for n in range(nb):
        g = lax.rem(n * 5 + head, nb)

        @pl.when(mine(g))
        def _():
            local(g).start()

        @pl.when(jnp.logical_not(mine(g)))
        def _():
            send(g).start()

    for g in range(nb):
        @pl.when(mine(g))
        def _():
            local(g).wait()

        @pl.when(jnp.logical_not(mine(g)))
        def _():
            send(g).wait_send()
    r = lax.rem(t, 4)
    core = lax.rem((r + 1) // 2, 2)
    for h in range(nb):
        here = jnp.logical_and(h == head, core == i)

        @pl.when(jnp.logical_not(here))
        def _():
            pltpu.make_async_remote_copy(
                src_ref=o_ref.at[0], dst_ref=out_ref.at[:, cols(h)], send_sem=ss.at[0], recv_sem=rs.at[h],
                device_id={'cp': c, 'tp': 2 * X + 1 - i}, device_id_type=MESH).wait_recv()


def spread(o, cp, tp):
    nb, rows, hd = o.shape
    vm = pl.BlockSpec(memory_space=pltpu.VMEM)
    dma = pltpu.SemaphoreType.DMA
    return pl.pallas_call(
        functools.partial(spread_kernel, cp, tp),
        out_shape=jax.ShapeDtypeStruct((rows, nb * hd), jnp.bfloat16),
        in_specs=[vm],
        out_specs=vm,
        scratch_shapes=[dma((nb,)), dma((nb,)), dma],
        compiler_params=pltpu.CompilerParams(collective_id=1, has_side_effects=True),
        name='spread',
    )(o)


CHIPS = ((2, 2), (1, 0), (0, 1), (3, 0), (0, 3), (1, 1), (3, 3), (1, 3), (3, 1), (2, 0), (0, 2), (2, 1), (1, 2), (2, 3), (3, 2), (0, 0))
GROUP = 4


def experts_kernel(cp, tp, send_ref, wg_hbm, wu_hbm, wd_hbm, back_ref, recv, z, wg, wu, wd,
                   ss, rs, sb, rb, sw, sl):
    c = lax.axis_index('cp')
    t = lax.axis_index('tp')
    nx = tp // 2
    X = t // 2
    i = lax.rem(t, 2)
    me = c * tp + t
    n_dev = cp * tp
    offs = [(a, b, k) for a, b in CHIPS for k in range(2) if (a, b, k) != (0, 0, 0)]
    weights = [pltpu.make_async_copy(h, v, sw.at[n]) for n, (h, v) in enumerate(((wg_hbm, wg), (wu_hbm, wu), (wd_hbm, wd)))]
    for w in weights:
        w.start()
    greet(cp, tp, c, t)

    def target(o):
        s = 1 - 2 * i
        return lax.rem(c + s * o[0] + cp, cp), 2 * lax.rem(X + s * o[1] + nx, nx) + lax.rem(i + o[2], 2)

    def origin(o):
        j = lax.rem(i + o[2], 2)
        s = 1 - 2 * j
        return lax.rem(c - s * o[0] + cp, cp), 2 * lax.rem(X - s * o[1] + nx, nx) + j

    def out(k):
        pc, pt = target(offs[k])
        return pltpu.make_async_remote_copy(
            src_ref=send_ref.at[pc * tp + pt], dst_ref=recv.at[k], send_sem=ss.at[k], recv_sem=rs.at[k],
            device_id={'cp': pc, 'tp': pt}, device_id_type=MESH)

    def home(k):
        pc, pt = origin(offs[k])
        return pltpu.make_async_remote_copy(
            src_ref=z.at[k], dst_ref=back_ref.at[me], send_sem=sb.at[k], recv_sem=rb.at[k],
            device_id={'cp': pc, 'tp': pt}, device_id_type=MESH)

    last = n_dev - 1
    for k in range(last):
        out(k).start()
    own = pltpu.make_async_copy(send_ref.at[me], recv.at[last], sl.at[0])
    own.start()
    for w in weights:
        w.wait()
    cap, hd = recv.shape[1:]

    def group(n, _):
        for k in range(last):
            @pl.when(n == k // GROUP)
            def _():
                out(k).wait_recv()

        @pl.when(n == last // GROUP)
        def _():
            own.wait()

        rows = recv[pl.ds(n * GROUP, GROUP)].reshape(GROUP * cap, hd)
        gg = jnp.dot(rows, wg[...], preferred_element_type=jnp.float32)
        uu = jnp.dot(rows, wu[...], preferred_element_type=jnp.float32)
        act = (gg * jax.nn.sigmoid(gg) * uu).astype(jnp.bfloat16)
        r = jnp.dot(act, wd[...], preferred_element_type=jnp.float32).astype(jnp.bfloat16)
        z[pl.ds(n * GROUP, GROUP)] = r.reshape(GROUP, cap, hd)
        for k in range(last):
            @pl.when(n == k // GROUP)
            def _():
                home(k).start()
        return 0

    lax.fori_loop(0, n_dev // GROUP, group, 0)
    keep = pltpu.make_async_copy(z.at[last], back_ref.at[me], sl.at[1])
    keep.start()
    for k in range(last):
        out(k).wait_send()
    for k in range(last):
        home(k).wait_send()
        home(k).wait_recv()
    keep.wait()


def experts(send, wg, wu, wd, cp, tp):
    anym = pl.BlockSpec(memory_space=pl.ANY)
    dma = pltpu.SemaphoreType.DMA
    n = send.shape[0]
    return pl.pallas_call(
        functools.partial(experts_kernel, cp, tp),
        out_shape=jax.ShapeDtypeStruct(send.shape, jnp.bfloat16),
        in_specs=[pl.BlockSpec(memory_space=pltpu.VMEM), anym, anym, anym],
        out_specs=pl.BlockSpec(memory_space=pltpu.VMEM),
        scratch_shapes=[
            pltpu.VMEM(send.shape, jnp.bfloat16), pltpu.VMEM(send.shape, jnp.bfloat16),
            pltpu.VMEM(wg.shape, jnp.bfloat16), pltpu.VMEM(wu.shape, jnp.bfloat16), pltpu.VMEM(wd.shape, jnp.bfloat16),
            dma((n,)), dma((n,)), dma((n,)), dma((n,)), dma((3,)), dma((2,)),
        ],
        compiler_params=pltpu.CompilerParams(collective_id=2, has_side_effects=True, vmem_limit_bytes=60 << 20),
        name='experts',
    )(send, wg, wu, wd)


def routes(idx, ne, cap):
    t = idx.shape[0]
    e = jnp.arange(ne)[None, :]
    o0 = (idx[:, 0:1] == e).astype(jnp.bfloat16)
    o1 = (idx[:, 1:2] == e).astype(jnp.bfloat16)
    tri = (jnp.arange(t)[:, None] >= jnp.arange(t)[None, :]).astype(jnp.bfloat16)
    both = jnp.dot(tri, jnp.concatenate([o0, o1], axis=1), preferred_element_type=jnp.float32)
    c0 = both[:, :ne]
    c1 = both[:, ne:] + both[t - 1:, :ne]
    s0 = jnp.sum(o0.astype(jnp.float32) * c0, axis=1).astype(jnp.int32) - 1
    s1 = jnp.sum(o1.astype(jnp.float32) * c1, axis=1).astype(jnp.int32) - 1
    return idx[:, 0] * cap + s0, idx[:, 1] * cap + s1


def solution(mesh):
    cp = mesh.shape['cp']
    tp = mesh.shape['tp']
    ne = cp * tp
    rows_spec = P(('dp', 'cp', 'tp'), None)
    exp_spec = P(('cp', 'tp'), None, None)

    def local(x, idx, gates, wq, wk, wv, wo, w1g, w1u, w2):
        t, hd = x.shape
        cap = 4 * t // ne
        d0, d1 = routes(idx, ne, cap)
        qkv = project_exchange(x, wq, wk, wv, cp, tp)
        qkv, wo = lax.optimization_barrier((qkv, wo))
        wo_all = lax.all_gather(wo, 'tp', axis=0, tiled=True)
        o = spread(attention(qkv), cp, tp)
        att = jnp.dot(o, wo_all, preferred_element_type=jnp.float32)
        h = (x.astype(jnp.float32) + att).astype(jnp.bfloat16)
        places = jnp.arange(ne * cap)
        pick = jnp.logical_or(places[:, None] == d0[None, :], places[:, None] == d1[None, :]).astype(jnp.bfloat16)
        send = jnp.dot(pick, h, preferred_element_type=jnp.float32).astype(jnp.bfloat16).reshape(ne, cap, hd)
        back = experts(send, w1g[0], w1u[0], w2[0], cp, tp).reshape(ne * cap, hd)
        z0 = jnp.dot((d0[:, None] == places[None, :]).astype(jnp.bfloat16), back, preferred_element_type=jnp.float32)
        z1 = jnp.dot((d1[:, None] == places[None, :]).astype(jnp.bfloat16), back, preferred_element_type=jnp.float32)
        y = h.astype(jnp.float32) + gates[:, 0:1] * z0 + gates[:, 1:2] * z1
        return y.astype(jnp.bfloat16)

    return jax.shard_map(local, mesh=mesh, in_specs=(rows_spec, rows_spec, rows_spec, P(None, 'tp'), P(None, 'tp'), P(None, 'tp'), P('tp', None), exp_spec, exp_spec, exp_spec), out_specs=rows_spec, check_vma=False)
```

```python
import functools

import jax
import jax.numpy as jnp
from jax import lax
from jax.experimental import pallas as pl
from jax.experimental.pallas import tpu as pltpu
from jax.sharding import PartitionSpec as P

HEAD_DIM = 128
NEG = -1e30
LOG2E = 1.4426950408889634
MESH = pl.DeviceIdType.MESH
HALF = 128
LAG = 4


def greet(cp, tp, c, t):
    sem = pltpu.get_barrier_semaphore()
    n = 0
    for dc in range(cp):
        for dt in range(tp):
            if dc or dt:
                peer = {'cp': lax.rem(c + dc, cp), 'tp': lax.rem(t + dt, tp)}
                pl.semaphore_signal(sem, inc=1, device_id=peer, device_id_type=MESH)
                n += 1
    pl.semaphore_wait(sem, n)


class Gather:
    def __init__(self, cp, tp, c, t, src, dst, send, passed, recv):
        self.c, self.t, self.nx = c, t, tp // 2
        self.X, self.i = t // 2, lax.rem(t, 2)
        self.partner = {'cp': c, 'tp': 2 * self.X + 1 - self.i}
        self.src, self.dst, self.send, self.passed, self.recv = src, dst, send, passed, recv

    def chip(self, d):
        return {'cp': self.c, 'tp': 2 * lax.rem(self.X + d, self.nx) + self.i}

    def source(self, u, w):
        dx = u + (u // 2) * (5 - 2 * u)
        return 2 * lax.rem(self.X + dx, self.nx) + lax.rem(self.i + w, 2)

    def copy(self, src, dst, send, u, w, hf, dev):
        return pltpu.make_async_remote_copy(
            src_ref=src, dst_ref=dst, send_sem=send, recv_sem=self.recv.at[u * 4 + w * 2 + hf],
            device_id=dev, device_id_type=MESH)

    def own(self, d, hf):
        dev, u, w = {0: (self.partner, 0, 1), 1: (self.chip(1), 2, 0), 3: (self.chip(3), 1, 0)}[d]
        return self.copy(self.src(hf), self.dst(self.t, hf), self.send.at[d * 2 + hf], u, w, hf, dev)

    def relay(self, hf):
        ref = self.dst(self.source(2 - hf, 0), hf)
        return self.copy(ref, ref, self.send.at[4 + hf], 3, 0, hf, self.chip(1 + 2 * hf))

    def share(self, u, hf):
        ref = self.dst(self.source(u, 0), hf)
        return self.copy(ref, ref, self.passed.at[u * 2 + hf], u, 1, hf, self.partner)

    def landed(self, u, w, hf):
        ref = self.dst(self.source(u, w), hf)
        return self.copy(ref, ref, self.passed.at[0], u, w, hf, self.partner)

    def start(self):
        for first in range(2):
            self.own(1, first).start()
            self.own(3, 1 - first).start()
            self.own(0, first).start()

    def drain(self):
        for hf in range(2):
            for d in (0, 1, 3):
                self.own(d, hf).wait_send()
            self.relay(hf).wait_send()
            for u in range(1, 4):
                self.share(u, hf).wait_send()


def project_kernel(cp, tp, x_hbm, wq_hbm, wk_hbm, wv_hbm, out_ref, xs, stage, wq_ref, wk_ref, wv_ref,
                   ss_x, ss_f, rs_x, sy, ry, sf, rf, sl, sw):
    c = lax.axis_index('cp')
    t = lax.axis_index('tp')
    X = t // 2
    i = lax.rem(t, 2)
    partner = {'cp': c, 'tp': 2 * X + 1 - i}
    main = i == c // 2
    loads = [pltpu.make_async_copy(h, v, sw.at[n]) for n, (h, v) in enumerate(
        ((x_hbm, xs.at[t]), (wq_hbm, wq_ref), (wk_hbm, wk_ref), (wv_hbm, wv_ref)))]
    for load in loads:
        load.start()
    greet(cp, tp, c, t)

    def rows(hf):
        return pl.ds(pl.multiple_of(hf * HALF, HALF), HALF)

    gather = Gather(cp, tp, c, t, lambda hf: x_hbm.at[rows(hf)], lambda s, hf: xs.at[s, rows(hf)], ss_x, ss_f, rs_x)
    source = gather.source

    def place(cc, s, hf):
        seg = cc + (s // 4) * (2 * cp - 1 - 2 * cc)
        return pl.ds(pl.multiple_of(seg * 1024 + lax.rem(s, 4) * 256 + hf * HALF, HALF), HALF)

    def piece(p):
        stage = p // 4
        w, v = lax.rem(p, 4) // 2, lax.rem(p, 2)
        first, last = (3 - stage) // 3, stage // 3
        mid = 1 - first - last
        return mid * (1 + v) + 3 * last, w, (1 - mid) * v + mid * lax.rem(stage + v, 2)

    def whose(p):
        u, w, hf = piece(p)
        return source(u, w), hf

    def y_send(p, kk, s, hf):
        return pltpu.make_async_remote_copy(
            src_ref=stage.at[p, kk], dst_ref=out_ref.at[place(c, s, hf)],
            send_sem=sy.at[p * 2 + kk], recv_sem=ry.at[c * 16 + p],
            device_id={'cp': 2 * i + kk, 'tp': t}, device_id_type=MESH)

    def keep(p, kk, s, hf):
        return pltpu.make_async_copy(stage.at[p, kk], out_ref.at[place(c, s, hf)], sl.at[p])

    def share(p, kk, s, hf):
        return pltpu.make_async_remote_copy(
            src_ref=stage.at[p, kk], dst_ref=out_ref.at[place(c, s, hf)],
            send_sem=sf.at[c * 16 + p], recv_sem=rf.at[c * 16 + p],
            device_id=partner, device_id_type=MESH)

    def pass_on(cc, p, s, hf):
        return pltpu.make_async_remote_copy(
            src_ref=out_ref.at[place(cc, s, hf)], dst_ref=out_ref.at[place(cc, s, hf)],
            send_sem=sf.at[cc * 16 + p], recv_sem=rf.at[cc * 16 + p],
            device_id=partner, device_id_type=MESH)

    def y_landed(cc, p, s, hf):
        return pltpu.make_async_remote_copy(
            src_ref=out_ref.at[place(cc, s, hf)], dst_ref=out_ref.at[place(cc, s, hf)],
            send_sem=sf.at[cc * 16 + p], recv_sem=ry.at[cc * 16 + p],
            device_id=partner, device_id_type=MESH)

    gather.start()
    for load in loads:
        load.wait()

    def project(xv, p, s, hf):
        for n, w_ref in enumerate((wq_ref, wk_ref, wv_ref)):
            r = jnp.dot(xv, w_ref[...], preferred_element_type=jnp.float32).astype(jnp.bfloat16)
            for kk in range(2):
                stage[p, kk, :, n * HEAD_DIM:(n + 1) * HEAD_DIM] = r[:, kk * HEAD_DIM:(kk + 1) * HEAD_DIM]
        for kk in range(2):
            here = c == 2 * i + kk

            @pl.when(jnp.logical_not(here))
            def _():
                y_send(p, kk, s, hf).start()

            @pl.when(here)
            def _():
                keep(p, kk, s, hf).start()
                share(p, kk, s, hf).start()

    def relay(p):
        s, hf = whose(p)

        @pl.when(main)
        def _():
            for d in range(1, cp):
                cc = lax.rem(c + d, cp)
                y_landed(cc, p, s, hf).wait_recv()
                pass_on(cc, p, s, hf).start()

    def step(p, _):
        u, w, hf = piece(p)
        for stage in range(1, 4):
            @pl.when(p == 4 * stage)
            def _():
                for v in range(2):
                    uu, _, hh = piece(4 * stage + v)
                    gather.landed(uu, 0, hh).wait_recv()
                    if stage == 1:
                        gather.relay(2 - uu).start()
                    gather.share(uu, hh).start()

        @pl.when(w == 1)
        def _():
            gather.landed(u, w, hf).wait_recv()

        s = source(u, w)
        project(xs[s, rows(hf), :], p, s, hf)

        @pl.when(p >= LAG)
        def _():
            relay(p - LAG)
        return 0

    lax.fori_loop(0, 16, step, 0)

    def tail(p, _):
        relay(p)
        return 0

    lax.fori_loop(16 - LAG, 16, tail, 0)
    gather.drain()

    def drain_pieces(p, _):
        s, hf = whose(p)
        for kk in range(2):
            here = c == 2 * i + kk

            @pl.when(jnp.logical_not(here))
            def _():
                y_send(p, kk, s, hf).wait_send()

            @pl.when(here)
            def _():
                keep(p, kk, s, hf).wait()

        @pl.when(main)
        def _():
            for cc in range(cp):
                pass_on(cc, p, s, hf).wait_send()

        @pl.when(jnp.logical_not(main))
        def _():
            for cc in range(cp):
                pass_on(cc, p, s, hf).wait_recv()
        return 0

    lax.fori_loop(0, 16, drain_pieces, 0)


def project_exchange(x, wq, wk, wv, cp, tp):
    seq = x.shape[0] * cp * tp
    hd = x.shape[1]
    anym = pl.BlockSpec(memory_space=pl.ANY)
    dma = pltpu.SemaphoreType.DMA
    return pl.pallas_call(
        functools.partial(project_kernel, cp, tp),
        out_shape=jax.ShapeDtypeStruct((seq, 3 * HEAD_DIM), jnp.bfloat16),
        in_specs=[anym] * 4,
        out_specs=anym,
        scratch_shapes=[
            pltpu.VMEM((tp,) + x.shape, jnp.bfloat16),
            pltpu.VMEM((16, 2, HALF, 3 * HEAD_DIM), jnp.bfloat16),
            pltpu.VMEM(wq.shape, jnp.bfloat16), pltpu.VMEM(wk.shape, jnp.bfloat16), pltpu.VMEM(wv.shape, jnp.bfloat16),
            dma((8,)), dma((8,)), dma((16,)), dma((32,)), dma((64,)), dma((64,)), dma((64,)), dma((16,)), dma((4,)),
        ],
        compiler_params=pltpu.CompilerParams(collective_id=0, has_side_effects=True, vmem_limit_bytes=62 << 20),
        name='project_exchange',
    )(x, wq, wk, wv)


QB = 256
KB = 1024


def q_block(g, i):
    return 4 * (g // 2) + (1 - i) * 3 * lax.rem(g, 2) + i * (1 + lax.rem(g, 2))


def attend_kernel(cp, tp, qkv_hbm, wo_hbm, x_hbm, h_ref, qkv_ref, wo, o_own, o_all, x_ref,
                  ss_w, ss_f, rs_w, ss, rs, sl, sq, sx):
    c = lax.axis_index('cp')
    t = lax.axis_index('tp')
    X = t // 2
    i = lax.rem(t, 2)
    head = X * cp + c
    nb = o_own.shape[0]
    nseg = nb // 2
    scale = HEAD_DIM ** -0.5 * LOG2E

    def seg_rows(j):
        return pl.ds(pl.multiple_of(j * KB, KB), KB)

    def load(j):
        return pltpu.make_async_copy(qkv_hbm.at[seg_rows(j)], qkv_ref.at[seg_rows(j)], sq.at[j])

    wrows = wo_hbm.shape[0]
    half = wrows // 2
    own_rows = pl.ds(pl.multiple_of(t * wrows, wrows), wrows)
    keep = pltpu.make_async_copy(wo_hbm, wo.at[own_rows], sx.at[0])
    keep.start()
    load_x = pltpu.make_async_copy(x_hbm, x_ref, sx.at[1])
    load_x.start()
    for j in range(nseg):
        load(j).start()
    greet(cp, tp, c, t)
    gather = Gather(
        cp, tp, c, t,
        lambda hf: wo_hbm.at[pl.ds(pl.multiple_of(hf * half, half), half)],
        lambda s, hf: wo.at[pl.ds(pl.multiple_of(s * wrows + hf * half, half), half)],
        ss_w, ss_f, rs_w)
    gather.start()

    def owner(g):
        b = q_block(g, i)
        seg = b // 4
        up = seg // cp
        return seg + up * (2 * cp - 1 - 2 * seg), lax.rem(b, 4) + 4 * up

    def cols(h):
        return pl.ds(pl.multiple_of(h * HEAD_DIM, HEAD_DIM), HEAD_DIM)

    def send(g):
        oc, ot = owner(g)
        return pltpu.make_async_remote_copy(
            src_ref=o_own.at[g], dst_ref=o_all.at[:, cols(head)], send_sem=ss.at[g], recv_sem=rs.at[head],
            device_id={'cp': oc, 'tp': ot}, device_id_type=MESH)

    def local(g):
        return pltpu.make_async_copy(o_own.at[g], o_all.at[:, cols(head)], sl)

    def mine(g):
        oc, ot = owner(g)
        return jnp.logical_and(oc == c, ot == t)

    def segment(seg, _):
        @pl.when(seg == nseg - 3)
        def _():
            for u in (1, 2):
                gather.landed(u, 0, 2 - u).wait_recv()
                gather.relay(2 - u).start()
                gather.share(u, 2 - u).start()

        @pl.when(seg == nseg - 2)
        def _():
            for u in (1, 2):
                gather.landed(u, 0, u - 1).wait_recv()
                gather.share(u, u - 1).start()

        load(seg).wait()
        blocks = [q_block(2 * seg + n, i) for n in range(2)]
        q = jnp.concatenate([qkv_ref[pl.ds(pl.multiple_of(b * QB, QB), QB), 0:HEAD_DIM] for b in blocks], axis=0)

        def chunk(j, m, l, acc, masked):
            k = qkv_ref[seg_rows(j), HEAD_DIM:2 * HEAD_DIM]
            v = qkv_ref[seg_rows(j), 2 * HEAD_DIM:3 * HEAD_DIM]
            s = lax.dot_general(q, k, (((1,), (1,)), ((), ())), preferred_element_type=jnp.float32) * scale
            if masked:
                row = lax.broadcasted_iota(jnp.int32, (2 * QB, KB), 0)
                qp = jnp.where(row < QB, blocks[0] * QB + row, (blocks[1] - 1) * QB + row)
                kp = j * KB + lax.broadcasted_iota(jnp.int32, (2 * QB, KB), 1)
                s = jnp.where(kp <= qp, s, NEG)
            mn = s[:, 0:128]
            for n in range(1, KB // 128):
                mn = jnp.maximum(mn, s[:, n * 128:(n + 1) * 128])
            mn = jnp.max(mn, axis=1, keepdims=True)
            if m is not None:
                mn = jnp.maximum(m, mn)
            w = jnp.exp2(s - mn)
            ls = w[:, 0:128]
            for n in range(1, KB // 128):
                ls = ls + w[:, n * 128:(n + 1) * 128]
            pv = jnp.dot(w.astype(jnp.bfloat16), v, preferred_element_type=jnp.float32)
            if m is None:
                return mn, ls, pv
            cc = jnp.exp2(m - mn)
            return mn, l * cc + ls, acc * cc + pv

        first = chunk(seg, None, None, None, True)
        m, l, acc = lax.fori_loop(0, seg, lambda j, carry: chunk(j, *carry, False), first)
        o = (acc / jnp.sum(l, axis=1, keepdims=True)).astype(jnp.bfloat16)
        for n in range(2):
            g = 2 * seg + n
            o_own[g] = o[n * QB:(n + 1) * QB]

            @pl.when(mine(g))
            def _():
                local(g).start()

            @pl.when(jnp.logical_not(mine(g)))
            def _():
                send(g).start()
        return 0

    lax.fori_loop(0, nseg, segment, 0)
    for hf in range(2):
        gather.landed(3, 0, hf).wait_recv()
        gather.share(3, hf).start()
    keep.wait()
    load_x.wait()
    for g in range(nb):
        @pl.when(mine(g))
        def _():
            local(g).wait()

        @pl.when(jnp.logical_not(mine(g)))
        def _():
            send(g).wait_send()
    core = lax.rem((lax.rem(t, 4) + 1) // 2, 2)
    for h in range(nb):
        here = jnp.logical_and(h == head, core == i)

        @pl.when(jnp.logical_not(here))
        def _():
            pltpu.make_async_remote_copy(
                src_ref=o_own.at[0], dst_ref=o_all.at[:, cols(h)], send_sem=ss.at[0], recv_sem=rs.at[h],
                device_id=gather.partner, device_id_type=MESH).wait_recv()
    for u in range(4):
        for hf in range(2):
            gather.landed(u, 1, hf).wait_recv()

    def column(n, _):
        at = pl.ds(pl.multiple_of(n * 256, 256), 256)
        att = jnp.dot(o_all[...], wo[:, at], preferred_element_type=jnp.float32)
        h_ref[:, at] = (x_ref[:, at].astype(jnp.float32) + att).astype(jnp.bfloat16)
        return 0

    lax.fori_loop(0, h_ref.shape[1] // 256, column, 0)
    gather.drain()


def attend(qkv, wo, x, cp, tp):
    seq = qkv.shape[0]
    nb = seq // QB // 2
    anym = pl.BlockSpec(memory_space=pl.ANY)
    dma = pltpu.SemaphoreType.DMA
    return pl.pallas_call(
        functools.partial(attend_kernel, cp, tp),
        out_shape=jax.ShapeDtypeStruct(x.shape, jnp.bfloat16),
        in_specs=[anym] * 3,
        out_specs=pl.BlockSpec(memory_space=pltpu.VMEM),
        scratch_shapes=[
            pltpu.VMEM(qkv.shape, jnp.bfloat16),
            pltpu.VMEM((tp * wo.shape[0], wo.shape[1]), jnp.bfloat16),
            pltpu.VMEM((nb, QB, HEAD_DIM), jnp.bfloat16),
            pltpu.VMEM((x.shape[0], nb * HEAD_DIM), jnp.bfloat16),
            pltpu.VMEM(x.shape, jnp.bfloat16),
            dma((8,)), dma((8,)), dma((16,)), dma((nb,)), dma((nb,)), dma, dma((nb // 2,)), dma((2,)),
        ],
        compiler_params=pltpu.CompilerParams(collective_id=1, has_side_effects=True, vmem_limit_bytes=62 << 20),
        name='attend',
    )(qkv, wo, x)


CHIPS = ((2, 2), (1, 0), (0, 1), (3, 0), (0, 3), (1, 1), (3, 3), (1, 3), (3, 1), (2, 0), (0, 2), (2, 1), (1, 2), (2, 3), (3, 2), (0, 0))
GROUP = 4


def experts_kernel(cp, tp, send_ref, wg_hbm, wu_hbm, wd_hbm, back_ref, recv, z, wg, wu, wd,
                   ss, rs, sb, rb, sw, sl):
    c = lax.axis_index('cp')
    t = lax.axis_index('tp')
    nx = tp // 2
    X = t // 2
    i = lax.rem(t, 2)
    me = c * tp + t
    n_dev = cp * tp
    offs = [(a, b, k) for a, b in CHIPS for k in range(2) if (a, b, k) != (0, 0, 0)]
    weights = [pltpu.make_async_copy(h, v, sw.at[n]) for n, (h, v) in enumerate(((wg_hbm, wg), (wu_hbm, wu), (wd_hbm, wd)))]
    for w in weights:
        w.start()
    greet(cp, tp, c, t)

    def target(o):
        s = 1 - 2 * i
        return lax.rem(c + s * o[0] + cp, cp), 2 * lax.rem(X + s * o[1] + nx, nx) + lax.rem(i + o[2], 2)

    def origin(o):
        j = lax.rem(i + o[2], 2)
        s = 1 - 2 * j
        return lax.rem(c - s * o[0] + cp, cp), 2 * lax.rem(X - s * o[1] + nx, nx) + j

    def out(k):
        pc, pt = target(offs[k])
        return pltpu.make_async_remote_copy(
            src_ref=send_ref.at[pc * tp + pt], dst_ref=recv.at[k], send_sem=ss.at[k], recv_sem=rs.at[k],
            device_id={'cp': pc, 'tp': pt}, device_id_type=MESH)

    def home(k):
        pc, pt = origin(offs[k])
        return pltpu.make_async_remote_copy(
            src_ref=z.at[k], dst_ref=back_ref.at[me], send_sem=sb.at[k], recv_sem=rb.at[k],
            device_id={'cp': pc, 'tp': pt}, device_id_type=MESH)

    last = n_dev - 1
    for k in range(last):
        out(k).start()
    own = pltpu.make_async_copy(send_ref.at[me], recv.at[last], sl.at[0])
    own.start()
    for w in weights:
        w.wait()
    cap, hd = recv.shape[1:]

    def group(n, _):
        for k in range(last):
            @pl.when(n == k // GROUP)
            def _():
                out(k).wait_recv()

        @pl.when(n == last // GROUP)
        def _():
            own.wait()

        rows = recv[pl.ds(n * GROUP, GROUP)].reshape(GROUP * cap, hd)
        gg = jnp.dot(rows, wg[...], preferred_element_type=jnp.float32)
        uu = jnp.dot(rows, wu[...], preferred_element_type=jnp.float32)
        act = (gg * jax.nn.sigmoid(gg) * uu).astype(jnp.bfloat16)
        r = jnp.dot(act, wd[...], preferred_element_type=jnp.float32).astype(jnp.bfloat16)
        z[pl.ds(n * GROUP, GROUP)] = r.reshape(GROUP, cap, hd)
        for k in range(last):
            @pl.when(n == k // GROUP)
            def _():
                home(k).start()
        return 0

    lax.fori_loop(0, n_dev // GROUP, group, 0)
    keep = pltpu.make_async_copy(z.at[last], back_ref.at[me], sl.at[1])
    keep.start()
    for k in range(last):
        out(k).wait_send()
    for k in range(last):
        home(k).wait_send()
        home(k).wait_recv()
    keep.wait()


def experts(send, wg, wu, wd, cp, tp):
    anym = pl.BlockSpec(memory_space=pl.ANY)
    dma = pltpu.SemaphoreType.DMA
    n = send.shape[0]
    return pl.pallas_call(
        functools.partial(experts_kernel, cp, tp),
        out_shape=jax.ShapeDtypeStruct(send.shape, jnp.bfloat16),
        in_specs=[pl.BlockSpec(memory_space=pltpu.VMEM), anym, anym, anym],
        out_specs=pl.BlockSpec(memory_space=pltpu.VMEM),
        scratch_shapes=[
            pltpu.VMEM(send.shape, jnp.bfloat16), pltpu.VMEM(send.shape, jnp.bfloat16),
            pltpu.VMEM(wg.shape, jnp.bfloat16), pltpu.VMEM(wu.shape, jnp.bfloat16), pltpu.VMEM(wd.shape, jnp.bfloat16),
            dma((n,)), dma((n,)), dma((n,)), dma((n,)), dma((3,)), dma((2,)),
        ],
        compiler_params=pltpu.CompilerParams(collective_id=2, has_side_effects=True, vmem_limit_bytes=60 << 20),
        name='experts',
    )(send, wg, wu, wd)


def routes(idx, ne, cap):
    t = idx.shape[0]
    e = jnp.arange(ne)[None, :]
    o0 = (idx[:, 0:1] == e).astype(jnp.bfloat16)
    o1 = (idx[:, 1:2] == e).astype(jnp.bfloat16)
    tri = (jnp.arange(t)[:, None] >= jnp.arange(t)[None, :]).astype(jnp.bfloat16)
    both = jnp.dot(tri, jnp.concatenate([o0, o1], axis=1), preferred_element_type=jnp.float32)
    c0 = both[:, :ne]
    c1 = both[:, ne:] + both[t - 1:, :ne]
    s0 = jnp.sum(o0.astype(jnp.float32) * c0, axis=1).astype(jnp.int32) - 1
    s1 = jnp.sum(o1.astype(jnp.float32) * c1, axis=1).astype(jnp.int32) - 1
    return idx[:, 0] * cap + s0, idx[:, 1] * cap + s1


def solution(mesh):
    cp = mesh.shape['cp']
    tp = mesh.shape['tp']
    ne = cp * tp
    rows_spec = P(('dp', 'cp', 'tp'), None)
    exp_spec = P(('cp', 'tp'), None, None)

    def local(x, idx, gates, wq, wk, wv, wo, w1g, w1u, w2):
        t, hd = x.shape
        cap = 4 * t // ne
        d0, d1 = routes(idx, ne, cap)
        qkv = project_exchange(x, wq, wk, wv, cp, tp)
        h = attend(qkv, wo, x, cp, tp)
        places = jnp.arange(ne * cap)
        pick = jnp.logical_or(places[:, None] == d0[None, :], places[:, None] == d1[None, :]).astype(jnp.bfloat16)
        send = jnp.dot(pick, h, preferred_element_type=jnp.float32).astype(jnp.bfloat16).reshape(ne, cap, hd)
        back = experts(send, w1g[0], w1u[0], w2[0], cp, tp).reshape(ne * cap, hd)
        z0 = jnp.dot((d0[:, None] == places[None, :]).astype(jnp.bfloat16), back, preferred_element_type=jnp.float32)
        z1 = jnp.dot((d1[:, None] == places[None, :]).astype(jnp.bfloat16), back, preferred_element_type=jnp.float32)
        y = h.astype(jnp.float32) + gates[:, 0:1] * z0 + gates[:, 1:2] * z1
        return y.astype(jnp.bfloat16)

    return jax.shard_map(local, mesh=mesh, in_specs=(rows_spec, rows_spec, rows_spec, P(None, 'tp'), P(None, 'tp'), P(None, 'tp'), P('tp', None), exp_spec, exp_spec, exp_spec), out_specs=rows_spec, check_vma=False)
```

```python
import functools

import jax
import jax.numpy as jnp
from jax import lax
from jax.experimental import pallas as pl
from jax.experimental.pallas import tpu as pltpu
from jax.sharding import PartitionSpec as P

HEAD_DIM = 128
NEG = -1e30
LOG2E = 1.4426950408889634
MESH = pl.DeviceIdType.MESH
PIECE = 64
LAG = 4


ORDER = (
    (2, 2, 0), (2, 2, 1), (1, 0, 0), (1, 0, 1), (0, 1, 0), (0, 1, 1), (3, 0, 0), (3, 0, 1),
    (0, 3, 0), (0, 3, 1), (1, 1, 0), (1, 1, 1), (3, 3, 0), (3, 3, 1), (1, 3, 0), (1, 3, 1),
    (3, 1, 0), (3, 1, 1), (2, 0, 0), (2, 0, 1), (0, 2, 0), (0, 2, 1), (2, 1, 0), (2, 1, 1),
    (1, 2, 0), (1, 2, 1), (2, 3, 0), (2, 3, 1), (3, 2, 0), (3, 2, 1), (0, 0, 1),
)


def target(o, cp, nx, c, t):
    X, i = t // 2, lax.rem(t, 2)
    s = 1 - 2 * i
    return lax.rem(c + s * o[0] + cp, cp), 2 * lax.rem(X + s * o[1] + nx, nx) + lax.rem(i + o[2], 2)


def origin(o, cp, nx, c, t):
    X, j = t // 2, lax.rem(t + o[2], 2)
    s = 1 - 2 * j
    return lax.rem(c - s * o[0] + cp, cp), 2 * lax.rem(X - s * o[1] + nx, nx) + j


def greet(cp, tp, c, t):
    sem = pltpu.get_barrier_semaphore()
    n = 0
    for dc in range(cp):
        for dt in range(tp):
            if dc or dt:
                peer = {'cp': lax.rem(c + dc, cp), 'tp': lax.rem(t + dt, tp)}
                pl.semaphore_signal(sem, inc=1, device_id=peer, device_id_type=MESH)
                n += 1
    pl.semaphore_wait(sem, n)


class Gather:
    def __init__(self, np, cp, tp, c, t, src, dst, send, relayed, passed, recv):
        self.np, self.c, self.t, self.nx = np, c, t, tp // 2
        self.X, self.i = t // 2, lax.rem(t, 2)
        self.partner = {'cp': c, 'tp': 2 * self.X + 1 - self.i}
        self.src, self.dst = src, dst
        self.send, self.relayed, self.passed, self.recv = send, relayed, passed, recv

    def chip(self, d):
        return {'cp': self.c, 'tp': 2 * lax.rem(self.X + d, self.nx) + self.i}

    def source(self, u, w):
        dx = u + (u // 2) * (5 - 2 * u)
        return 2 * lax.rem(self.X + dx, self.nx) + lax.rem(self.i + w, 2)

    def copy(self, src, dst, send, u, w, pc, dev):
        return pltpu.make_async_remote_copy(
            src_ref=src, dst_ref=dst, send_sem=send, recv_sem=self.recv.at[(u * 2 + w) * self.np + pc],
            device_id=dev, device_id_type=MESH)

    def own(self, d, pc):
        dev, u, w = {0: (self.partner, 0, 1), 1: (self.chip(1), 2, 0), 2: (self.chip(3), 1, 0)}[d]
        return self.copy(self.src(pc), self.dst(self.t, pc), self.send.at[d * self.np + pc], u, w, pc, dev)

    def relay(self, pc):
        back = pc // (self.np // 2)
        ref = self.dst(self.source(2 - back, 0), pc)
        return self.copy(ref, ref, self.relayed.at[pc], 3, 0, pc, self.chip(1 + 2 * back))

    def share(self, u, pc):
        ref = self.dst(self.source(u, 0), pc)
        return self.copy(ref, ref, self.passed.at[(u - 1) * self.np + pc], u, 1, pc, self.partner)

    def landed(self, u, w, pc):
        ref = self.dst(self.source(u, w), pc)
        return self.copy(ref, ref, self.passed.at[0], u, w, pc, self.partner)

    def start(self):
        for n in range(self.np):
            self.own(1, n).start()
            self.own(2, self.np - 1 - n).start()
            self.own(0, n).start()

    def drain(self):
        for pc in range(self.np):
            for d in range(3):
                self.own(d, pc).wait_send()
            self.relay(pc).wait_send()
            for u in range(1, 4):
                self.share(u, pc).wait_send()

    @staticmethod
    def semaphores(np):
        dma = pltpu.SemaphoreType.DMA
        return [dma((3 * np,)), dma((np,)), dma((3 * np,)), dma((8 * np,))]


def route(cp, tp, c, t, idx_ref, place_ref, turned_ref):
    n_dev = cp * tp
    rows, choices = idx_ref.shape[1], 2
    cap = 2 * choices * rows // n_dev
    names = jnp.where(lax.broadcasted_iota(jnp.int32, idx_ref.shape, 0) < choices, idx_ref[...], 0).astype(jnp.float32).T
    lane = lax.broadcasted_iota(jnp.int32, (rows, 128), 1)
    named = [(lane.astype(jnp.float32) == names[:, n:n + 1]).astype(jnp.float32) for n in range(choices)]
    tri = (lax.broadcasted_iota(jnp.int32, (rows, rows), 0) >= lax.broadcasted_iota(jnp.int32, (rows, rows), 1))
    count = jnp.dot(tri.astype(jnp.float32).astype(jnp.bfloat16), jnp.concatenate(named, axis=1).astype(jnp.bfloat16),
                    preferred_element_type=jnp.float32)
    one = lax.broadcasted_iota(jnp.int32, (8, 128), 1)
    base = jnp.where(one == c * tp + t, float((n_dev - 1) * cap), 0.0)
    for k, o in enumerate(ORDER):
        pc, pt = target(o, cp, tp // 2, c, t)
        base = jnp.where(one == pc * tp + pt, float(k * cap), base)
    base = base[0:1, :]
    later = base + count[rows - 1:rows, :128]
    p0 = jnp.sum(named[0] * (count[:, :128] + base), axis=1, keepdims=True) - 1.0
    p1 = jnp.sum(named[1] * (count[:, 128:] + later), axis=1, keepdims=True) - 1.0
    both = jnp.where(lane == 0, p0, jnp.where(lane == 1, p1, 0.0))
    place_ref[...] = both
    turned_ref[...] = both.T[:8, :]


def project_kernel(cp, tp, x_hbm, idx_hbm, wq_hbm, wk_hbm, wv_hbm, out_ref, place_ref, turned_ref, xs, stage, wq_ref, wk_ref, wv_ref, idx_ref,
                   ss_x, sr_x, ss_f, rs_x, sy, ry, sf, rf, sl, sw):
    c = lax.axis_index('cp')
    t = lax.axis_index('tp')
    X = t // 2
    i = lax.rem(t, 2)
    partner = {'cp': c, 'tp': 2 * X + 1 - i}
    main = i == c // 2
    loads = [pltpu.make_async_copy(h, v, sw.at[n]) for n, (h, v) in enumerate(
        ((x_hbm, xs.at[t]), (wq_hbm, wq_ref), (wk_hbm, wk_ref), (wv_hbm, wv_ref), (idx_hbm, idx_ref.at[0:2])))]
    for load in loads:
        load.start()
    greet(cp, tp, c, t)

    np = x_hbm.shape[0] // PIECE
    total = tp * np

    def rows(hf):
        return pl.ds(pl.multiple_of(hf * PIECE, PIECE), PIECE)

    gather = Gather(
        np, cp, tp, c, t, lambda hf: x_hbm.at[rows(hf)], lambda s, hf: xs.at[s, rows(hf)], ss_x, sr_x, ss_f, rs_x)
    source = gather.source

    def place(cc, s, hf):
        seg = cc + (s // (tp // 2)) * (2 * cp - 1 - 2 * cc)
        return pl.ds(pl.multiple_of((seg * (tp // 2) + lax.rem(s, tp // 2)) * (np * PIECE) + hf * PIECE, PIECE), PIECE)

    def piece(p):
        eighth = p // 8
        own, opp = 1 - (eighth + 3) // 4, eighth // 3
        mid = 1 - own - opp
        k = p // 4 - 2
        v = lax.rem(p, 2)
        w = own * (p // 4) + (1 - own) * (lax.rem(p, 4) // 2)
        pc = own * lax.rem(p, 4) + mid * ((1 - v) * (3 - k) + v * k) + opp * ((1 - v) * (k - 4) + v * (7 - k))
        return mid * (1 + v) + 3 * opp, w, pc

    def whose(p):
        u, w, hf = piece(p)
        return source(u, w), hf

    def y_send(p, kk, s, hf):
        return pltpu.make_async_remote_copy(
            src_ref=stage.at[p, kk], dst_ref=out_ref.at[place(c, s, hf)],
            send_sem=sy.at[p * 2 + kk], recv_sem=ry.at[c * total + p],
            device_id={'cp': 2 * i + kk, 'tp': t}, device_id_type=MESH)

    def keep(p, kk, s, hf):
        return pltpu.make_async_copy(stage.at[p, kk], out_ref.at[place(c, s, hf)], sl.at[p])

    def share(p, kk, s, hf):
        return pltpu.make_async_remote_copy(
            src_ref=stage.at[p, kk], dst_ref=out_ref.at[place(c, s, hf)],
            send_sem=sf.at[c * total + p], recv_sem=rf.at[c * total + p],
            device_id=partner, device_id_type=MESH)

    def pass_on(cc, p, s, hf):
        return pltpu.make_async_remote_copy(
            src_ref=out_ref.at[place(cc, s, hf)], dst_ref=out_ref.at[place(cc, s, hf)],
            send_sem=sf.at[cc * total + p], recv_sem=rf.at[cc * total + p],
            device_id=partner, device_id_type=MESH)

    def y_landed(cc, p, s, hf):
        return pltpu.make_async_remote_copy(
            src_ref=out_ref.at[place(cc, s, hf)], dst_ref=out_ref.at[place(cc, s, hf)],
            send_sem=sf.at[cc * total + p], recv_sem=ry.at[cc * total + p],
            device_id=partner, device_id_type=MESH)

    gather.start()
    for load in loads:
        load.wait()
    route(cp, tp, c, t, idx_ref, place_ref, turned_ref)

    def project(xv, p, s, hf):
        for n, w_ref in enumerate((wq_ref, wk_ref, wv_ref)):
            r = jnp.dot(xv, w_ref[...], preferred_element_type=jnp.float32).astype(jnp.bfloat16)
            for kk in range(2):
                stage[p, kk, :, n * HEAD_DIM:(n + 1) * HEAD_DIM] = r[:, kk * HEAD_DIM:(kk + 1) * HEAD_DIM]
        for kk in range(2):
            here = c == 2 * i + kk

            @pl.when(jnp.logical_not(here))
            def _():
                y_send(p, kk, s, hf).start()

            @pl.when(here)
            def _():
                keep(p, kk, s, hf).start()
                share(p, kk, s, hf).start()

    def relay(p):
        s, hf = whose(p)

        @pl.when(main)
        def _():
            for d in range(1, cp):
                cc = lax.rem(c + d, cp)
                y_landed(cc, p, s, hf).wait_recv()
                pass_on(cc, p, s, hf).start()

    def step(p, _):
        u, w, hf = piece(p)
        for first in range(8, total, 4):
            @pl.when(p == first)
            def _():
                for v in range(2):
                    uu, _, pc = piece(first + v)
                    gather.landed(uu, 0, pc).wait_recv()
                    if first < 16:
                        gather.relay(pc).start()
                    gather.share(uu, pc).start()

        @pl.when(w == 1)
        def _():
            gather.landed(u, w, hf).wait_recv()

        s = source(u, w)
        project(xs[s, rows(hf), :], p, s, hf)

        @pl.when(p >= LAG)
        def _():
            relay(p - LAG)
        return 0

    lax.fori_loop(0, total, step, 0)

    def tail(p, _):
        relay(p)
        return 0

    lax.fori_loop(total - LAG, total, tail, 0)
    gather.drain()

    def drain_pieces(p, _):
        s, hf = whose(p)
        for kk in range(2):
            here = c == 2 * i + kk

            @pl.when(jnp.logical_not(here))
            def _():
                y_send(p, kk, s, hf).wait_send()

            @pl.when(here)
            def _():
                keep(p, kk, s, hf).wait()

        @pl.when(main)
        def _():
            for cc in range(cp):
                pass_on(cc, p, s, hf).wait_send()

        @pl.when(jnp.logical_not(main))
        def _():
            for cc in range(cp):
                pass_on(cc, p, s, hf).wait_recv()
        return 0

    lax.fori_loop(0, total, drain_pieces, 0)


def project_exchange(x, idx, wq, wk, wv, cp, tp):
    seq = x.shape[0] * cp * tp
    np = x.shape[0] // PIECE
    total = tp * np
    anym = pl.BlockSpec(memory_space=pl.ANY)
    dma = pltpu.SemaphoreType.DMA
    return pl.pallas_call(
        functools.partial(project_kernel, cp, tp),
        out_shape=(
            jax.ShapeDtypeStruct((seq, 3 * HEAD_DIM), jnp.bfloat16),
            jax.ShapeDtypeStruct((x.shape[0], 128), jnp.float32),
            jax.ShapeDtypeStruct((8, x.shape[0]), jnp.float32),
        ),
        in_specs=[anym] * 5,
        out_specs=(anym, pl.BlockSpec(memory_space=pltpu.VMEM), pl.BlockSpec(memory_space=pltpu.VMEM)),
        scratch_shapes=[
            pltpu.VMEM((tp,) + x.shape, jnp.bfloat16),
            pltpu.VMEM((total, 2, PIECE, 3 * HEAD_DIM), jnp.bfloat16),
            pltpu.VMEM(wq.shape, jnp.bfloat16), pltpu.VMEM(wk.shape, jnp.bfloat16), pltpu.VMEM(wv.shape, jnp.bfloat16),
            pltpu.VMEM((8, x.shape[0]), jnp.int32),
            *Gather.semaphores(np),
            dma((2 * total,)), dma((cp * total,)), dma((cp * total,)), dma((cp * total,)), dma((total,)), dma((5,)),
        ],
        compiler_params=pltpu.CompilerParams(collective_id=0, has_side_effects=True, vmem_limit_bytes=62 << 20),
        name='project_exchange',
    )(x, idx.T, wq, wk, wv)


QB = 256
KB = 1024


def q_block(g, i):
    return 4 * (g // 2) + (1 - i) * 3 * lax.rem(g, 2) + i * (1 + lax.rem(g, 2))


def attend_kernel(cp, tp, qkv_hbm, wo_hbm, x_hbm, h_ref, qkv_ref, wo, o_own, o_all, x_ref,
                  ss_w, sr_w, ss_f, rs_w, ss, rs, sl, sq, sx):
    c = lax.axis_index('cp')
    t = lax.axis_index('tp')
    X = t // 2
    i = lax.rem(t, 2)
    head = X * cp + c
    nb = o_own.shape[0]
    nseg = nb // 2
    scale = HEAD_DIM ** -0.5 * LOG2E

    def seg_rows(j):
        return pl.ds(pl.multiple_of(j * KB, KB), KB)

    def load(j):
        return pltpu.make_async_copy(qkv_hbm.at[seg_rows(j)], qkv_ref.at[seg_rows(j)], sq.at[j])

    wrows = wo_hbm.shape[0]
    half = wrows // 2
    own_rows = pl.ds(pl.multiple_of(t * wrows, wrows), wrows)
    keep = pltpu.make_async_copy(wo_hbm, wo.at[own_rows], sx.at[0])
    keep.start()
    load_x = pltpu.make_async_copy(x_hbm, x_ref, sx.at[1])
    load_x.start()
    for j in range(nseg):
        load(j).start()
    greet(cp, tp, c, t)
    gather = Gather(
        2, cp, tp, c, t,
        lambda hf: wo_hbm.at[pl.ds(pl.multiple_of(hf * half, half), half)],
        lambda s, hf: wo.at[pl.ds(pl.multiple_of(s * wrows + hf * half, half), half)],
        ss_w, sr_w, ss_f, rs_w)
    gather.start()

    def owner(g):
        b = q_block(g, i)
        seg = b // 4
        up = seg // cp
        return seg + up * (2 * cp - 1 - 2 * seg), lax.rem(b, 4) + 4 * up

    def cols(h):
        return pl.ds(pl.multiple_of(h * HEAD_DIM, HEAD_DIM), HEAD_DIM)

    def send(g):
        oc, ot = owner(g)
        return pltpu.make_async_remote_copy(
            src_ref=o_own.at[g], dst_ref=o_all.at[:, cols(head)], send_sem=ss.at[g], recv_sem=rs.at[head],
            device_id={'cp': oc, 'tp': ot}, device_id_type=MESH)

    def local(g):
        return pltpu.make_async_copy(o_own.at[g], o_all.at[:, cols(head)], sl)

    def mine(g):
        oc, ot = owner(g)
        return jnp.logical_and(oc == c, ot == t)

    def segment(seg, _):
        @pl.when(seg == nseg - 3)
        def _():
            for u in (1, 2):
                gather.landed(u, 0, 2 - u).wait_recv()
                gather.relay(2 - u).start()
                gather.share(u, 2 - u).start()

        @pl.when(seg == nseg - 2)
        def _():
            for u in (1, 2):
                gather.landed(u, 0, u - 1).wait_recv()
                gather.share(u, u - 1).start()

        load(seg).wait()
        blocks = [q_block(2 * seg + n, i) for n in range(2)]
        q = jnp.concatenate([qkv_ref[pl.ds(pl.multiple_of(b * QB, QB), QB), 0:HEAD_DIM] for b in blocks], axis=0)

        def chunk(j, m, l, acc, masked):
            k = qkv_ref[seg_rows(j), HEAD_DIM:2 * HEAD_DIM]
            v = qkv_ref[seg_rows(j), 2 * HEAD_DIM:3 * HEAD_DIM]
            s = lax.dot_general(q, k, (((1,), (1,)), ((), ())), preferred_element_type=jnp.float32) * scale
            if masked:
                row = lax.broadcasted_iota(jnp.int32, (2 * QB, KB), 0)
                qp = jnp.where(row < QB, blocks[0] * QB + row, (blocks[1] - 1) * QB + row)
                kp = j * KB + lax.broadcasted_iota(jnp.int32, (2 * QB, KB), 1)
                s = jnp.where(kp <= qp, s, NEG)
            mn = s[:, 0:128]
            for n in range(1, KB // 128):
                mn = jnp.maximum(mn, s[:, n * 128:(n + 1) * 128])
            mn = jnp.max(mn, axis=1, keepdims=True)
            if m is not None:
                mn = jnp.maximum(m, mn)
            w = jnp.exp2(s - mn)
            ls = w[:, 0:128]
            for n in range(1, KB // 128):
                ls = ls + w[:, n * 128:(n + 1) * 128]
            pv = jnp.dot(w.astype(jnp.bfloat16), v, preferred_element_type=jnp.float32)
            if m is None:
                return mn, ls, pv
            cc = jnp.exp2(m - mn)
            return mn, l * cc + ls, acc * cc + pv

        first = chunk(seg, None, None, None, True)
        m, l, acc = lax.fori_loop(0, seg, lambda j, carry: chunk(j, *carry, False), first)
        o = (acc / jnp.sum(l, axis=1, keepdims=True)).astype(jnp.bfloat16)
        for n in range(2):
            g = 2 * seg + n
            o_own[g] = o[n * QB:(n + 1) * QB]

            @pl.when(mine(g))
            def _():
                local(g).start()

            @pl.when(jnp.logical_not(mine(g)))
            def _():
                send(g).start()
        return 0

    lax.fori_loop(0, nseg, segment, 0)
    for hf in range(2):
        gather.landed(3, 0, hf).wait_recv()
        gather.share(3, hf).start()
    keep.wait()
    load_x.wait()
    for g in range(nb):
        @pl.when(mine(g))
        def _():
            local(g).wait()

        @pl.when(jnp.logical_not(mine(g)))
        def _():
            send(g).wait_send()
    core = lax.rem((lax.rem(t, 4) + 1) // 2, 2)
    for h in range(nb):
        here = jnp.logical_and(h == head, core == i)

        @pl.when(jnp.logical_not(here))
        def _():
            pltpu.make_async_remote_copy(
                src_ref=o_own.at[0], dst_ref=o_all.at[:, cols(h)], send_sem=ss.at[0], recv_sem=rs.at[h],
                device_id=gather.partner, device_id_type=MESH).wait_recv()
    for u in range(4):
        for hf in range(2):
            gather.landed(u, 1, hf).wait_recv()

    def column(n, _):
        at = pl.ds(pl.multiple_of(n * 256, 256), 256)
        att = jnp.dot(o_all[...], wo[:, at], preferred_element_type=jnp.float32)
        h_ref[:, at] = (x_ref[:, at].astype(jnp.float32) + att).astype(jnp.bfloat16)
        return 0

    lax.fori_loop(0, h_ref.shape[1] // 256, column, 0)
    gather.drain()


def attend(qkv, wo, x, cp, tp):
    seq = qkv.shape[0]
    nb = seq // QB // 2
    anym = pl.BlockSpec(memory_space=pl.ANY)
    dma = pltpu.SemaphoreType.DMA
    return pl.pallas_call(
        functools.partial(attend_kernel, cp, tp),
        out_shape=jax.ShapeDtypeStruct(x.shape, jnp.bfloat16),
        in_specs=[anym] * 3,
        out_specs=pl.BlockSpec(memory_space=pltpu.VMEM),
        scratch_shapes=[
            pltpu.VMEM(qkv.shape, jnp.bfloat16),
            pltpu.VMEM((tp * wo.shape[0], wo.shape[1]), jnp.bfloat16),
            pltpu.VMEM((nb, QB, HEAD_DIM), jnp.bfloat16),
            pltpu.VMEM((x.shape[0], nb * HEAD_DIM), jnp.bfloat16),
            pltpu.VMEM(x.shape, jnp.bfloat16),
            *Gather.semaphores(2), dma((nb,)), dma((nb,)), dma, dma((nb // 2,)), dma((2,)),
        ],
        compiler_params=pltpu.CompilerParams(collective_id=1, has_side_effects=True, vmem_limit_bytes=62 << 20),
        name='attend',
    )(qkv, wo, x)


GROUP = 4
PICK = 4
PUT = 4


def experts_kernel(cp, tp, turned_hbm, place_hbm, gates_hbm, h_ref, wg_hbm, wu_hbm, wd_hbm, out_ref,
                   send, recv, z, back, wg, wu, wd, d_row, d_col, gates_ref, y_ref,
                   ss, rs, sb, rb, sw, sl):
    c = lax.axis_index('cp')
    t = lax.axis_index('tp')
    nx = tp // 2
    X = t // 2
    i = lax.rem(t, 2)
    me = c * tp + t
    n_dev = cp * tp
    cap, hd = recv.shape[1:]
    rows = h_ref.shape[0]
    last = n_dev - 1
    small = [pltpu.make_async_copy(h, v, sw.at[3 + n]) for n, (h, v) in enumerate(
        ((turned_hbm, d_row), (place_hbm, d_col), (gates_hbm, gates_ref.at[0:2])))]
    weights = [pltpu.make_async_copy(h, v, sw.at[n]) for n, (h, v) in enumerate(((wg_hbm, wg), (wu_hbm, wu), (wd_hbm, wd)))]
    for w in small + weights:
        w.start()
    for w in small:
        w.wait()

    def out(k):
        pc, pt = target(ORDER[k], cp, nx, c, t)
        return pltpu.make_async_remote_copy(
            src_ref=send.at[k], dst_ref=recv.at[k], send_sem=ss.at[k], recv_sem=rs.at[k],
            device_id={'cp': pc, 'tp': pt}, device_id_type=MESH)

    def home(k):
        pc, pt = origin(ORDER[k], cp, nx, c, t)
        return pltpu.make_async_remote_copy(
            src_ref=z.at[k], dst_ref=back.at[k], send_sem=sb.at[k], recv_sem=rb.at[k],
            device_id={'cp': pc, 'tp': pt}, device_id_type=MESH)

    def places(n, blocks, axis, shape):
        return (n * blocks * cap + lax.broadcasted_iota(jnp.int32, shape, axis)).astype(jnp.float32)

    def select(n, _):
        at = places(n, PICK, 0, (PICK * cap, rows))
        pick = jnp.logical_or(at == d_row[0:1, :], at == d_row[1:2, :]).astype(jnp.float32).astype(jnp.bfloat16)
        r = jnp.dot(pick, h_ref[...], preferred_element_type=jnp.float32).astype(jnp.bfloat16)
        send[pl.ds(n * PICK, PICK)] = r.reshape(PICK, cap, hd)

        @pl.when(n == 0)
        def _():
            greet(cp, tp, c, t)

        for k in range(last):
            @pl.when(n == k // PICK)
            def _():
                out(k).start()
        return 0

    lax.fori_loop(0, n_dev // PICK, select, 0)
    own = pltpu.make_async_copy(send.at[last], recv.at[last], sl.at[0])
    own.start()
    for w in weights:
        w.wait()

    def group(n, _):
        for k in range(last):
            @pl.when(n == k // GROUP)
            def _():
                out(k).wait_recv()

        @pl.when(n == last // GROUP)
        def _():
            own.wait()

        xr = recv[pl.ds(n * GROUP, GROUP)].reshape(GROUP * cap, hd)
        gg = jnp.dot(xr, wg[...], preferred_element_type=jnp.float32)
        uu = jnp.dot(xr, wu[...], preferred_element_type=jnp.float32)
        act = (gg * jax.nn.sigmoid(gg) * uu).astype(jnp.bfloat16)
        r = jnp.dot(act, wd[...], preferred_element_type=jnp.float32).astype(jnp.bfloat16)
        z[pl.ds(n * GROUP, GROUP)] = r.reshape(GROUP, cap, hd)
        for k in range(last):
            @pl.when(n == k // GROUP)
            def _():
                home(k).start()
        return 0

    lax.fori_loop(0, n_dev // GROUP, group, 0)
    keep = pltpu.make_async_copy(z.at[last], back.at[last], sl.at[1])
    keep.start()
    y_ref[...] = h_ref[...].astype(jnp.float32)
    gates = jnp.where(lax.broadcasted_iota(jnp.int32, gates_ref.shape, 0) < 2, gates_ref[...], 0.0).T
    for k in range(last):
        out(k).wait_send()

    def combine(n, _):
        for k in range(last):
            @pl.when(n == k // PUT)
            def _():
                home(k).wait_recv()

        @pl.when(n == last // PUT)
        def _():
            keep.wait()

        at = places(n, PUT, 1, (rows, PUT * cap))
        blk = back[pl.ds(n * PUT, PUT)].reshape(PUT * cap, hd)
        total = y_ref[...]
        for choice in range(2):
            put = (at == d_col[:, choice:choice + 1]).astype(jnp.float32).astype(jnp.bfloat16)
            zz = jnp.dot(put, blk, preferred_element_type=jnp.float32)
            total = total + gates[:, choice:choice + 1] * zz
        y_ref[...] = total
        return 0

    lax.fori_loop(0, n_dev // PUT, combine, 0)
    out_ref[...] = y_ref[...].astype(jnp.bfloat16)
    for k in range(last):
        home(k).wait_send()


def experts(place, turned, gates, h, wg, wu, wd, cp, tp):
    anym = pl.BlockSpec(memory_space=pl.ANY)
    vm = pl.BlockSpec(memory_space=pltpu.VMEM)
    dma = pltpu.SemaphoreType.DMA
    n = cp * tp
    cap = 2 * gates.shape[1] * h.shape[0] // n
    blocks = pltpu.VMEM((n, cap, h.shape[1]), jnp.bfloat16)
    return pl.pallas_call(
        functools.partial(experts_kernel, cp, tp),
        out_shape=jax.ShapeDtypeStruct(h.shape, jnp.bfloat16),
        in_specs=[anym, anym, anym, vm, anym, anym, anym],
        out_specs=vm,
        scratch_shapes=[
            blocks, blocks, blocks, blocks,
            pltpu.VMEM(wg.shape, jnp.bfloat16), pltpu.VMEM(wu.shape, jnp.bfloat16), pltpu.VMEM(wd.shape, jnp.bfloat16),
            pltpu.VMEM(turned.shape, jnp.float32), pltpu.VMEM(place.shape, jnp.float32), pltpu.VMEM((8, h.shape[0]), jnp.float32),
            pltpu.VMEM(h.shape, jnp.float32),
            dma((n,)), dma((n,)), dma((n,)), dma((n,)), dma((6,)), dma((2,)),
        ],
        compiler_params=pltpu.CompilerParams(collective_id=2, has_side_effects=True, vmem_limit_bytes=62 << 20),
        name='experts',
    )(turned, place, gates.T, h, wg, wu, wd)


def solution(mesh):
    cp = mesh.shape['cp']
    tp = mesh.shape['tp']
    rows_spec = P(('dp', 'cp', 'tp'), None)
    exp_spec = P(('cp', 'tp'), None, None)

    def local(x, idx, gates, wq, wk, wv, wo, w1g, w1u, w2):
        qkv, place, turned = project_exchange(x, idx, wq, wk, wv, cp, tp)
        h = attend(qkv, wo, x, cp, tp)
        return experts(place, turned, gates, h, w1g[0], w1u[0], w2[0], cp, tp)

    return jax.shard_map(local, mesh=mesh, in_specs=(rows_spec, rows_spec, rows_spec, P(None, 'tp'), P(None, 'tp'), P(None, 'tp'), P('tp', None), exp_spec, exp_spec, exp_spec), out_specs=rows_spec, check_vma=False)
```

```python
import functools

import jax
import jax.numpy as jnp
from jax import lax
from jax.experimental import pallas as pl
from jax.experimental.pallas import tpu as pltpu
from jax.sharding import PartitionSpec as P

HEAD_DIM = 128
NEG = -1e30
LOG2E = 1.4426950408889634
MESH = pl.DeviceIdType.MESH
PIECE = 64
LAG = 4


ORDER = (
    (2, 2, 0), (2, 2, 1), (1, 0, 0), (1, 0, 1), (0, 1, 0), (0, 1, 1), (3, 0, 0), (3, 0, 1),
    (0, 3, 0), (0, 3, 1), (1, 1, 0), (1, 1, 1), (3, 3, 0), (3, 3, 1), (1, 3, 0), (1, 3, 1),
    (3, 1, 0), (3, 1, 1), (2, 0, 0), (2, 0, 1), (0, 2, 0), (0, 2, 1), (2, 1, 0), (2, 1, 1),
    (1, 2, 0), (1, 2, 1), (2, 3, 0), (2, 3, 1), (3, 2, 0), (3, 2, 1), (0, 0, 1),
)


def target(o, cp, nx, c, t):
    X, i = t // 2, lax.rem(t, 2)
    s = 1 - 2 * i
    return lax.rem(c + s * o[0] + cp, cp), 2 * lax.rem(X + s * o[1] + nx, nx) + lax.rem(i + o[2], 2)


def origin(o, cp, nx, c, t):
    X, j = t // 2, lax.rem(t + o[2], 2)
    s = 1 - 2 * j
    return lax.rem(c - s * o[0] + cp, cp), 2 * lax.rem(X - s * o[1] + nx, nx) + j


def meet(peers):
    sem = pltpu.get_barrier_semaphore()
    for pc, pt in peers:
        pl.semaphore_signal(sem, inc=1, device_id={'cp': pc, 'tp': pt}, device_id_type=MESH)
    pl.semaphore_wait(sem, len(peers))


def greet(cp, tp, c, t):
    meet([(lax.rem(c + dc, cp), lax.rem(t + dt, tp)) for dc in range(cp) for dt in range(tp) if dc or dt])


class Gather:
    def __init__(self, np, cp, tp, c, t, src, dst, send, relayed, passed, recv):
        self.np, self.c, self.t, self.nx = np, c, t, tp // 2
        self.X, self.i = t // 2, lax.rem(t, 2)
        self.partner = {'cp': c, 'tp': 2 * self.X + 1 - self.i}
        self.src, self.dst = src, dst
        self.send, self.relayed, self.passed, self.recv = send, relayed, passed, recv

    def chip(self, d):
        return {'cp': self.c, 'tp': 2 * lax.rem(self.X + d, self.nx) + self.i}

    def source(self, u, w):
        dx = u + (u // 2) * (5 - 2 * u)
        return 2 * lax.rem(self.X + dx, self.nx) + lax.rem(self.i + w, 2)

    def copy(self, src, dst, send, u, w, pc, dev):
        return pltpu.make_async_remote_copy(
            src_ref=src, dst_ref=dst, send_sem=send, recv_sem=self.recv.at[(u * 2 + w) * self.np + pc],
            device_id=dev, device_id_type=MESH)

    def own(self, d, pc):
        dev, u, w = {0: (self.partner, 0, 1), 1: (self.chip(1), 2, 0), 2: (self.chip(3), 1, 0)}[d]
        return self.copy(self.src(pc), self.dst(self.t, pc), self.send.at[d * self.np + pc], u, w, pc, dev)

    def relay(self, pc):
        back = pc // (self.np // 2)
        ref = self.dst(self.source(2 - back, 0), pc)
        return self.copy(ref, ref, self.relayed.at[pc], 3, 0, pc, self.chip(1 + 2 * back))

    def share(self, u, pc):
        ref = self.dst(self.source(u, 0), pc)
        return self.copy(ref, ref, self.passed.at[(u - 1) * self.np + pc], u, 1, pc, self.partner)

    def landed(self, u, w, pc):
        ref = self.dst(self.source(u, w), pc)
        return self.copy(ref, ref, self.passed.at[0], u, w, pc, self.partner)

    def start(self):
        for n in range(self.np):
            self.own(1, n).start()
            self.own(2, self.np - 1 - n).start()
            self.own(0, n).start()

    def drain(self):
        for pc in range(self.np):
            for d in range(3):
                self.own(d, pc).wait_send()
            self.relay(pc).wait_send()
            for u in range(1, 4):
                self.share(u, pc).wait_send()

    @staticmethod
    def semaphores(np):
        dma = pltpu.SemaphoreType.DMA
        return [dma((3 * np,)), dma((np,)), dma((3 * np,)), dma((8 * np,))]


def route(cp, tp, c, t, idx_ref, place_ref, turned_ref):
    n_dev = cp * tp
    rows, choices = idx_ref.shape[1], 2
    cap = 2 * choices * rows // n_dev
    names = jnp.where(lax.broadcasted_iota(jnp.int32, idx_ref.shape, 0) < choices, idx_ref[...], 0).astype(jnp.float32).T
    lane = lax.broadcasted_iota(jnp.int32, (rows, 128), 1)
    named = [(lane.astype(jnp.float32) == names[:, n:n + 1]).astype(jnp.float32) for n in range(choices)]
    tri = (lax.broadcasted_iota(jnp.int32, (rows, rows), 0) >= lax.broadcasted_iota(jnp.int32, (rows, rows), 1))
    count = jnp.dot(tri.astype(jnp.float32).astype(jnp.bfloat16), jnp.concatenate(named, axis=1).astype(jnp.bfloat16),
                    preferred_element_type=jnp.float32)
    one = lax.broadcasted_iota(jnp.int32, (8, 128), 1)
    base = jnp.where(one == c * tp + t, float((n_dev - 1) * cap), 0.0)
    for k, o in enumerate(ORDER):
        pc, pt = target(o, cp, tp // 2, c, t)
        base = jnp.where(one == pc * tp + pt, float(k * cap), base)
    base = base[0:1, :]
    later = base + count[rows - 1:rows, :128]
    p0 = jnp.sum(named[0] * (count[:, :128] + base), axis=1, keepdims=True) - 1.0
    p1 = jnp.sum(named[1] * (count[:, 128:] + later), axis=1, keepdims=True) - 1.0
    both = jnp.where(lane == 0, p0, jnp.where(lane == 1, p1, 0.0))
    place_ref[...] = both
    turned_ref[...] = both.T[:8, :]


def project_kernel(cp, tp, x_hbm, idx_hbm, wq_hbm, wk_hbm, wv_hbm, out_ref, place_ref, turned_ref, xs, stage, wq_ref, wk_ref, wv_ref, idx_ref,
                   ss_x, sr_x, ss_f, rs_x, sy, ry, sf, rf, sl, sw):
    c = lax.axis_index('cp')
    t = lax.axis_index('tp')
    X = t // 2
    i = lax.rem(t, 2)
    partner = {'cp': c, 'tp': 2 * X + 1 - i}
    main = i == c // 2
    loads = [pltpu.make_async_copy(h, v, sw.at[n]) for n, (h, v) in enumerate(
        ((x_hbm, xs.at[t]), (wq_hbm, wq_ref), (wk_hbm, wk_ref), (wv_hbm, wv_ref), (idx_hbm, idx_ref.at[0:2])))]
    for load in loads:
        load.start()
    meet([(c, lax.rem(t + 2, tp)), (c, lax.rem(t + tp - 2, tp)), (c, 2 * X + 1 - i)]
         + [(lax.rem(c + d, cp), t) for d in range(1, cp)])

    np = x_hbm.shape[0] // PIECE
    total = tp * np

    def rows(hf):
        return pl.ds(pl.multiple_of(hf * PIECE, PIECE), PIECE)

    gather = Gather(
        np, cp, tp, c, t, lambda hf: x_hbm.at[rows(hf)], lambda s, hf: xs.at[s, rows(hf)], ss_x, sr_x, ss_f, rs_x)
    source = gather.source

    def place(cc, s, hf):
        seg = cc + (s // (tp // 2)) * (2 * cp - 1 - 2 * cc)
        return pl.ds(pl.multiple_of((seg * (tp // 2) + lax.rem(s, tp // 2)) * (np * PIECE) + hf * PIECE, PIECE), PIECE)

    def piece(p):
        eighth = p // 8
        own, opp = 1 - (eighth + 3) // 4, eighth // 3
        mid = 1 - own - opp
        k = p // 4 - 2
        v = lax.rem(p, 2)
        w = own * (p // 4) + (1 - own) * (lax.rem(p, 4) // 2)
        pc = own * lax.rem(p, 4) + mid * ((1 - v) * (3 - k) + v * k) + opp * ((1 - v) * (k - 4) + v * (7 - k))
        return mid * (1 + v) + 3 * opp, w, pc

    def whose(p):
        u, w, hf = piece(p)
        return source(u, w), hf

    def y_send(p, kk, s, hf):
        return pltpu.make_async_remote_copy(
            src_ref=stage.at[p, kk], dst_ref=out_ref.at[place(c, s, hf)],
            send_sem=sy.at[p * 2 + kk], recv_sem=ry.at[c * total + p],
            device_id={'cp': 2 * i + kk, 'tp': t}, device_id_type=MESH)

    def keep(p, kk, s, hf):
        return pltpu.make_async_copy(stage.at[p, kk], out_ref.at[place(c, s, hf)], sl.at[p])

    def share(p, kk, s, hf):
        return pltpu.make_async_remote_copy(
            src_ref=stage.at[p, kk], dst_ref=out_ref.at[place(c, s, hf)],
            send_sem=sf.at[c * total + p], recv_sem=rf.at[c * total + p],
            device_id=partner, device_id_type=MESH)

    def pass_on(cc, p, s, hf):
        return pltpu.make_async_remote_copy(
            src_ref=out_ref.at[place(cc, s, hf)], dst_ref=out_ref.at[place(cc, s, hf)],
            send_sem=sf.at[cc * total + p], recv_sem=rf.at[cc * total + p],
            device_id=partner, device_id_type=MESH)

    def y_landed(cc, p, s, hf):
        return pltpu.make_async_remote_copy(
            src_ref=out_ref.at[place(cc, s, hf)], dst_ref=out_ref.at[place(cc, s, hf)],
            send_sem=sf.at[cc * total + p], recv_sem=ry.at[cc * total + p],
            device_id=partner, device_id_type=MESH)

    gather.start()
    for load in loads:
        load.wait()
    route(cp, tp, c, t, idx_ref, place_ref, turned_ref)

    def project(xv, p, s, hf):
        for n, w_ref in enumerate((wq_ref, wk_ref, wv_ref)):
            r = jnp.dot(xv, w_ref[...], preferred_element_type=jnp.float32).astype(jnp.bfloat16)
            for kk in range(2):
                stage[p, kk, :, n * HEAD_DIM:(n + 1) * HEAD_DIM] = r[:, kk * HEAD_DIM:(kk + 1) * HEAD_DIM]
        for kk in range(2):
            here = c == 2 * i + kk

            @pl.when(jnp.logical_not(here))
            def _():
                y_send(p, kk, s, hf).start()

            @pl.when(here)
            def _():
                keep(p, kk, s, hf).start()
                share(p, kk, s, hf).start()

    def relay(p):
        s, hf = whose(p)

        @pl.when(main)
        def _():
            for d in range(1, cp):
                cc = lax.rem(c + d, cp)
                y_landed(cc, p, s, hf).wait_recv()
                pass_on(cc, p, s, hf).start()

    def step(p, _):
        u, w, hf = piece(p)
        for first in range(8, total, 4):
            @pl.when(p == first)
            def _():
                for v in range(2):
                    uu, _, pc = piece(first + v)
                    gather.landed(uu, 0, pc).wait_recv()
                    if first < 16:
                        gather.relay(pc).start()
                    gather.share(uu, pc).start()

        @pl.when(w == 1)
        def _():
            gather.landed(u, w, hf).wait_recv()

        s = source(u, w)
        project(xs[s, rows(hf), :], p, s, hf)

        @pl.when(p >= LAG)
        def _():
            relay(p - LAG)
        return 0

    lax.fori_loop(0, total, step, 0)

    def tail(p, _):
        relay(p)
        return 0

    lax.fori_loop(total - LAG, total, tail, 0)
    gather.drain()

    def drain_pieces(p, _):
        s, hf = whose(p)
        for kk in range(2):
            here = c == 2 * i + kk

            @pl.when(jnp.logical_not(here))
            def _():
                y_send(p, kk, s, hf).wait_send()

            @pl.when(here)
            def _():
                keep(p, kk, s, hf).wait()

        @pl.when(main)
        def _():
            for cc in range(cp):
                pass_on(cc, p, s, hf).wait_send()

        @pl.when(jnp.logical_not(main))
        def _():
            for cc in range(cp):
                pass_on(cc, p, s, hf).wait_recv()
        return 0

    lax.fori_loop(0, total, drain_pieces, 0)


def project_exchange(x, idx, wq, wk, wv, cp, tp):
    seq = x.shape[0] * cp * tp
    np = x.shape[0] // PIECE
    total = tp * np
    anym = pl.BlockSpec(memory_space=pl.ANY)
    dma = pltpu.SemaphoreType.DMA
    return pl.pallas_call(
        functools.partial(project_kernel, cp, tp),
        out_shape=(
            jax.ShapeDtypeStruct((seq, 3 * HEAD_DIM), jnp.bfloat16),
            jax.ShapeDtypeStruct((x.shape[0], 128), jnp.float32),
            jax.ShapeDtypeStruct((8, x.shape[0]), jnp.float32),
        ),
        in_specs=[anym] * 5,
        out_specs=(anym, pl.BlockSpec(memory_space=pltpu.VMEM), pl.BlockSpec(memory_space=pltpu.VMEM)),
        scratch_shapes=[
            pltpu.VMEM((tp,) + x.shape, jnp.bfloat16),
            pltpu.VMEM((total, 2, PIECE, 3 * HEAD_DIM), jnp.bfloat16),
            pltpu.VMEM(wq.shape, jnp.bfloat16), pltpu.VMEM(wk.shape, jnp.bfloat16), pltpu.VMEM(wv.shape, jnp.bfloat16),
            pltpu.VMEM((8, x.shape[0]), jnp.int32),
            *Gather.semaphores(np),
            dma((2 * total,)), dma((cp * total,)), dma((cp * total,)), dma((cp * total,)), dma((total,)), dma((5,)),
        ],
        compiler_params=pltpu.CompilerParams(collective_id=0, has_side_effects=True, vmem_limit_bytes=62 << 20),
        name='project_exchange',
    )(x, idx.T, wq, wk, wv)


QB = 256
KB = 1024


def q_block(g, i):
    return 4 * (g // 2) + (1 - i) * 3 * lax.rem(g, 2) + i * (1 + lax.rem(g, 2))


def attend_kernel(cp, tp, qkv_hbm, wo_hbm, x_hbm, h_ref, qkv_ref, wo, o_own, o_all, x_ref,
                  ss_w, sr_w, ss_f, rs_w, ss, rs, sl, sq, sx):
    c = lax.axis_index('cp')
    t = lax.axis_index('tp')
    X = t // 2
    i = lax.rem(t, 2)
    head = X * cp + c
    nb = o_own.shape[0]
    nseg = nb // 2
    scale = HEAD_DIM ** -0.5 * LOG2E

    def seg_rows(j):
        return pl.ds(pl.multiple_of(j * KB, KB), KB)

    def load(j):
        return pltpu.make_async_copy(qkv_hbm.at[seg_rows(j)], qkv_ref.at[seg_rows(j)], sq.at[j])

    wrows = wo_hbm.shape[0]
    half = wrows // 2
    own_rows = pl.ds(pl.multiple_of(t * wrows, wrows), wrows)
    keep = pltpu.make_async_copy(wo_hbm, wo.at[own_rows], sx.at[0])
    keep.start()
    load_x = pltpu.make_async_copy(x_hbm, x_ref, sx.at[1])
    load_x.start()
    for j in range(nseg):
        load(j).start()
    greet(cp, tp, c, t)
    gather = Gather(
        2, cp, tp, c, t,
        lambda hf: wo_hbm.at[pl.ds(pl.multiple_of(hf * half, half), half)],
        lambda s, hf: wo.at[pl.ds(pl.multiple_of(s * wrows + hf * half, half), half)],
        ss_w, sr_w, ss_f, rs_w)
    gather.start()

    def owner(g):
        b = q_block(g, i)
        seg = b // 4
        up = seg // cp
        return seg + up * (2 * cp - 1 - 2 * seg), lax.rem(b, 4) + 4 * up

    def cols(h):
        return pl.ds(pl.multiple_of(h * HEAD_DIM, HEAD_DIM), HEAD_DIM)

    def send(g):
        oc, ot = owner(g)
        return pltpu.make_async_remote_copy(
            src_ref=o_own.at[g], dst_ref=o_all.at[:, cols(head)], send_sem=ss.at[g], recv_sem=rs.at[head],
            device_id={'cp': oc, 'tp': ot}, device_id_type=MESH)

    def local(g):
        return pltpu.make_async_copy(o_own.at[g], o_all.at[:, cols(head)], sl)

    def mine(g):
        oc, ot = owner(g)
        return jnp.logical_and(oc == c, ot == t)

    def segment(seg, _):
        @pl.when(seg == nseg - 3)
        def _():
            for u in (1, 2):
                gather.landed(u, 0, 2 - u).wait_recv()
                gather.relay(2 - u).start()
                gather.share(u, 2 - u).start()

        @pl.when(seg == nseg - 2)
        def _():
            for u in (1, 2):
                gather.landed(u, 0, u - 1).wait_recv()
                gather.share(u, u - 1).start()

        load(seg).wait()
        blocks = [q_block(2 * seg + n, i) for n in range(2)]
        q = jnp.concatenate([qkv_ref[pl.ds(pl.multiple_of(b * QB, QB), QB), 0:HEAD_DIM] for b in blocks], axis=0)

        def chunk(j, m, l, acc, masked):
            k = qkv_ref[seg_rows(j), HEAD_DIM:2 * HEAD_DIM]
            v = qkv_ref[seg_rows(j), 2 * HEAD_DIM:3 * HEAD_DIM]
            s = lax.dot_general(q, k, (((1,), (1,)), ((), ())), preferred_element_type=jnp.float32) * scale
            if masked:
                row = lax.broadcasted_iota(jnp.int32, (2 * QB, KB), 0)
                qp = jnp.where(row < QB, blocks[0] * QB + row, (blocks[1] - 1) * QB + row)
                kp = j * KB + lax.broadcasted_iota(jnp.int32, (2 * QB, KB), 1)
                s = jnp.where(kp <= qp, s, NEG)
            mn = s[:, 0:128]
            for n in range(1, KB // 128):
                mn = jnp.maximum(mn, s[:, n * 128:(n + 1) * 128])
            mn = jnp.max(mn, axis=1, keepdims=True)
            if m is not None:
                mn = jnp.maximum(m, mn)
            w = jnp.exp2(s - mn)
            ls = w[:, 0:128]
            for n in range(1, KB // 128):
                ls = ls + w[:, n * 128:(n + 1) * 128]
            pv = jnp.dot(w.astype(jnp.bfloat16), v, preferred_element_type=jnp.float32)
            if m is None:
                return mn, ls, pv
            cc = jnp.exp2(m - mn)
            return mn, l * cc + ls, acc * cc + pv

        first = chunk(seg, None, None, None, True)
        m, l, acc = lax.fori_loop(0, seg, lambda j, carry: chunk(j, *carry, False), first)
        o = (acc / jnp.sum(l, axis=1, keepdims=True)).astype(jnp.bfloat16)
        for n in range(2):
            g = 2 * seg + n
            o_own[g] = o[n * QB:(n + 1) * QB]

            @pl.when(mine(g))
            def _():
                local(g).start()

            @pl.when(jnp.logical_not(mine(g)))
            def _():
                send(g).start()
        return 0

    lax.fori_loop(0, nseg, segment, 0)
    for hf in range(2):
        gather.landed(3, 0, hf).wait_recv()
        gather.share(3, hf).start()
    keep.wait()
    load_x.wait()
    for g in range(nb):
        @pl.when(mine(g))
        def _():
            local(g).wait()

        @pl.when(jnp.logical_not(mine(g)))
        def _():
            send(g).wait_send()
    core = lax.rem((lax.rem(t, 4) + 1) // 2, 2)
    for h in range(nb):
        here = jnp.logical_and(h == head, core == i)

        @pl.when(jnp.logical_not(here))
        def _():
            pltpu.make_async_remote_copy(
                src_ref=o_own.at[0], dst_ref=o_all.at[:, cols(h)], send_sem=ss.at[0], recv_sem=rs.at[h],
                device_id=gather.partner, device_id_type=MESH).wait_recv()
    for u in range(4):
        for hf in range(2):
            gather.landed(u, 1, hf).wait_recv()

    def column(n, _):
        at = pl.ds(pl.multiple_of(n * 256, 256), 256)
        att = jnp.dot(o_all[...], wo[:, at], preferred_element_type=jnp.float32)
        h_ref[:, at] = (x_ref[:, at].astype(jnp.float32) + att).astype(jnp.bfloat16)
        return 0

    lax.fori_loop(0, h_ref.shape[1] // 256, column, 0)
    gather.drain()


def attend(qkv, wo, x, cp, tp):
    seq = qkv.shape[0]
    nb = seq // QB // 2
    anym = pl.BlockSpec(memory_space=pl.ANY)
    dma = pltpu.SemaphoreType.DMA
    return pl.pallas_call(
        functools.partial(attend_kernel, cp, tp),
        out_shape=jax.ShapeDtypeStruct(x.shape, jnp.bfloat16),
        in_specs=[anym] * 3,
        out_specs=pl.BlockSpec(memory_space=pltpu.VMEM),
        scratch_shapes=[
            pltpu.VMEM(qkv.shape, jnp.bfloat16),
            pltpu.VMEM((tp * wo.shape[0], wo.shape[1]), jnp.bfloat16),
            pltpu.VMEM((nb, QB, HEAD_DIM), jnp.bfloat16),
            pltpu.VMEM((x.shape[0], nb * HEAD_DIM), jnp.bfloat16),
            pltpu.VMEM(x.shape, jnp.bfloat16),
            *Gather.semaphores(2), dma((nb,)), dma((nb,)), dma, dma((nb // 2,)), dma((2,)),
        ],
        compiler_params=pltpu.CompilerParams(collective_id=1, has_side_effects=True, vmem_limit_bytes=62 << 20),
        name='attend',
    )(qkv, wo, x)


GROUP = 4
PICK = 4
PUT = 4


def experts_kernel(cp, tp, turned_hbm, place_hbm, gates_hbm, h_ref, wg_hbm, wu_hbm, wd_hbm, out_ref,
                   send, recv, z, back, wg, wu, wd, d_row, d_col, gates_ref, y_ref,
                   ss, rs, sb, rb, sw, sl):
    c = lax.axis_index('cp')
    t = lax.axis_index('tp')
    nx = tp // 2
    X = t // 2
    i = lax.rem(t, 2)
    me = c * tp + t
    n_dev = cp * tp
    cap, hd = recv.shape[1:]
    rows = h_ref.shape[0]
    last = n_dev - 1
    small = [pltpu.make_async_copy(h, v, sw.at[3 + n]) for n, (h, v) in enumerate(
        ((turned_hbm, d_row), (place_hbm, d_col), (gates_hbm, gates_ref.at[0:2])))]
    weights = [pltpu.make_async_copy(h, v, sw.at[n]) for n, (h, v) in enumerate(((wg_hbm, wg), (wu_hbm, wu), (wd_hbm, wd)))]
    for w in small + weights:
        w.start()
    for w in small:
        w.wait()

    def out(k):
        pc, pt = target(ORDER[k], cp, nx, c, t)
        return pltpu.make_async_remote_copy(
            src_ref=send.at[k], dst_ref=recv.at[k], send_sem=ss.at[k], recv_sem=rs.at[k],
            device_id={'cp': pc, 'tp': pt}, device_id_type=MESH)

    def home(k):
        pc, pt = origin(ORDER[k], cp, nx, c, t)
        return pltpu.make_async_remote_copy(
            src_ref=z.at[k], dst_ref=back.at[k], send_sem=sb.at[k], recv_sem=rb.at[k],
            device_id={'cp': pc, 'tp': pt}, device_id_type=MESH)

    def places(n, blocks, axis, shape):
        return (n * blocks * cap + lax.broadcasted_iota(jnp.int32, shape, axis)).astype(jnp.float32)

    def select(n, _):
        at = places(n, PICK, 0, (PICK * cap, rows))
        pick = jnp.logical_or(at == d_row[0:1, :], at == d_row[1:2, :]).astype(jnp.float32).astype(jnp.bfloat16)
        r = jnp.dot(pick, h_ref[...], preferred_element_type=jnp.float32).astype(jnp.bfloat16)
        send[pl.ds(n * PICK, PICK)] = r.reshape(PICK, cap, hd)

        @pl.when(n == 0)
        def _():
            greet(cp, tp, c, t)

        for k in range(last):
            @pl.when(n == k // PICK)
            def _():
                out(k).start()
        return 0

    lax.fori_loop(0, n_dev // PICK, select, 0)
    own = pltpu.make_async_copy(send.at[last], recv.at[last], sl.at[0])
    own.start()
    for w in weights:
        w.wait()

    def group(n, _):
        for k in range(last):
            @pl.when(n == k // GROUP)
            def _():
                out(k).wait_recv()

        @pl.when(n == last // GROUP)
        def _():
            own.wait()

        xr = recv[pl.ds(n * GROUP, GROUP)].reshape(GROUP * cap, hd)
        gg = jnp.dot(xr, wg[...], preferred_element_type=jnp.float32)
        uu = jnp.dot(xr, wu[...], preferred_element_type=jnp.float32)
        act = (gg * jax.nn.sigmoid(gg) * uu).astype(jnp.bfloat16)
        r = jnp.dot(act, wd[...], preferred_element_type=jnp.float32).astype(jnp.bfloat16)
        z[pl.ds(n * GROUP, GROUP)] = r.reshape(GROUP, cap, hd)
        for k in range(last):
            @pl.when(n == k // GROUP)
            def _():
                home(k).start()
        return 0

    lax.fori_loop(0, n_dev // GROUP, group, 0)
    keep = pltpu.make_async_copy(z.at[last], back.at[last], sl.at[1])
    keep.start()
    y_ref[...] = h_ref[...].astype(jnp.float32)
    gates = jnp.where(lax.broadcasted_iota(jnp.int32, gates_ref.shape, 0) < 2, gates_ref[...], 0.0).T
    for k in range(last):
        out(k).wait_send()

    def combine(n, _):
        for k in range(last):
            @pl.when(n == k // PUT)
            def _():
                home(k).wait_recv()

        @pl.when(n == last // PUT)
        def _():
            keep.wait()

        at = places(n, PUT, 1, (rows, PUT * cap))
        blk = back[pl.ds(n * PUT, PUT)].reshape(PUT * cap, hd)
        total = y_ref[...]
        for choice in range(2):
            put = (at == d_col[:, choice:choice + 1]).astype(jnp.float32).astype(jnp.bfloat16)
            zz = jnp.dot(put, blk, preferred_element_type=jnp.float32)
            total = total + gates[:, choice:choice + 1] * zz
        y_ref[...] = total
        return 0

    lax.fori_loop(0, n_dev // PUT, combine, 0)
    out_ref[...] = y_ref[...].astype(jnp.bfloat16)
    for k in range(last):
        home(k).wait_send()


def experts(place, turned, gates, h, wg, wu, wd, cp, tp):
    anym = pl.BlockSpec(memory_space=pl.ANY)
    vm = pl.BlockSpec(memory_space=pltpu.VMEM)
    dma = pltpu.SemaphoreType.DMA
    n = cp * tp
    cap = 2 * gates.shape[1] * h.shape[0] // n
    blocks = pltpu.VMEM((n, cap, h.shape[1]), jnp.bfloat16)
    return pl.pallas_call(
        functools.partial(experts_kernel, cp, tp),
        out_shape=jax.ShapeDtypeStruct(h.shape, jnp.bfloat16),
        in_specs=[anym, anym, anym, vm, anym, anym, anym],
        out_specs=vm,
        scratch_shapes=[
            blocks, blocks, blocks, blocks,
            pltpu.VMEM(wg.shape, jnp.bfloat16), pltpu.VMEM(wu.shape, jnp.bfloat16), pltpu.VMEM(wd.shape, jnp.bfloat16),
            pltpu.VMEM(turned.shape, jnp.float32), pltpu.VMEM(place.shape, jnp.float32), pltpu.VMEM((8, h.shape[0]), jnp.float32),
            pltpu.VMEM(h.shape, jnp.float32),
            dma((n,)), dma((n,)), dma((n,)), dma((n,)), dma((6,)), dma((2,)),
        ],
        compiler_params=pltpu.CompilerParams(collective_id=2, has_side_effects=True, vmem_limit_bytes=62 << 20),
        name='experts',
    )(turned, place, gates.T, h, wg, wu, wd)


def solution(mesh):
    cp = mesh.shape['cp']
    tp = mesh.shape['tp']
    rows_spec = P(('dp', 'cp', 'tp'), None)
    exp_spec = P(('cp', 'tp'), None, None)

    def local(x, idx, gates, wq, wk, wv, wo, w1g, w1u, w2):
        qkv, place, turned = project_exchange(x, idx, wq, wk, wv, cp, tp)
        h = attend(qkv, wo, x, cp, tp)
        return experts(place, turned, gates, h, w1g[0], w1u[0], w2[0], cp, tp)

    return jax.shard_map(local, mesh=mesh, in_specs=(rows_spec, rows_spec, rows_spec, P(None, 'tp'), P(None, 'tp'), P(None, 'tp'), P('tp', None), exp_spec, exp_spec, exp_spec), out_specs=rows_spec, check_vma=False)
```
